16 devices in a mesh: data: 2 (over y, z), seq: 8 (over x, core).
Axes of the slice: x: 4, y: 2, z: 1, core: 2. Of those that a mesh axis runs over, the one named last changes fastest.
The devices are a block of a 4x4x8 slice.
Arguments:
- x_tok: bfloat16 [32768, 768], P(('data', 'seq')), parts along dimension 0
- dy_tok: bfloat16 [32768, 768], P(('data', 'seq')), parts along dimension 0
- ln_gamma: float32 [768], replicated
- ln_beta: float32 [768], replicated
- w_qkv: bfloat16 [768, 3, 16, 48], replicated
- w_out: bfloat16 [768, 768], replicated
Outputs:
- output 1: bfloat16 [32768, 768], P(('data', 'seq')), parts along dimension 0
- output 2: bfloat16 [32768, 768], P(('data', 'seq')), parts along dimension 0
- output 3: float32 [1536, 3, 16, 48], P(('data', 'seq')), parts along dimension 0
- output 4: float32 [1536, 768], P(('data', 'seq')), parts along dimension 0
- output 5: float32 [1536], P('data'), parts along dimension 0
- output 6: float32 [1536], P('data'), parts along dimension 0
There are 2 independent parts. The reference program is written for one: setup_inputs(seed, part) draws one part's arguments, and reference() takes and returns one part's arrays. A program takes and returns all parts, laid end to end along the dimension named above; an argument that names none is the same for every part.
All inputs are finite; a program needn't handle non-finite values.
Results may differ from the reference program's by a relative error of at most 0.00480294.
Values are sent between devices in bfloat16 or wider.
A program may use at most 768 MiB of HBM per device.

```python
import jax
import jax.numpy as jnp
from jax import lax

TOKENS_DEV = 2048
SEQ = 8
D = 768
HEADS = 16
HEAD = D // HEADS
TOKENS = SEQ * TOKENS_DEV
LN_EPS = 1e-5


def setup_inputs(seed: int = 0, part: int = 0) -> dict:
    part_key = jax.random.fold_in(jax.random.key(seed), part)
    keys_part = jax.random.split(part_key, 5)
    keys_shared = jax.random.split(jax.random.key(seed + 1), 4)
    noise = jax.random.normal(keys_part[0], (SEQ, TOKENS_DEV, D), jnp.float32)
    shard_offs = jax.random.normal(keys_part[1], (SEQ, 1, D), jnp.float32)
    base_offs = 0.7 * jax.random.normal(keys_part[2], (1, 1, D), jnp.float32)
    x_tok = (noise + shard_offs + base_offs).reshape(TOKENS, D).astype(jnp.bfloat16)
    grad_mean = 0.5 * jax.random.normal(keys_part[3], (1, D), jnp.float32)
    dy_tok = (jax.random.normal(keys_part[4], (TOKENS, D), jnp.float32) + grad_mean).astype(jnp.bfloat16)
    ln_gamma = 1.0 + 0.3 * jax.random.normal(keys_shared[0], (D,), jnp.float32)
    ln_beta = 0.5 * jax.random.normal(keys_shared[1], (D,), jnp.float32)
    w_qkv = (jax.random.normal(keys_shared[2], (D, 3, HEADS, HEAD), jnp.float32) * D ** -0.5).astype(jnp.bfloat16)
    w_out = (jax.random.normal(keys_shared[3], (D, D), jnp.float32) * D ** -0.5).astype(jnp.bfloat16)
    return {"x_tok": x_tok, "dy_tok": dy_tok, "ln_gamma": ln_gamma, "ln_beta": ln_beta, "w_qkv": w_qkv, "w_out": w_out}


def phi_act(t):
    return jnp.where(t > 0, t + 1.0, jnp.exp(jnp.minimum(t, 0.0)))


def phi_slope(t):
    return jnp.where(t > 0, 1.0, jnp.exp(jnp.minimum(t, 0.0)))


def reference(x_tok, dy_tok, ln_gamma, ln_beta, w_qkv, w_out):
    x_f32 = x_tok.astype(jnp.float32)
    centered = x_f32 - jnp.mean(x_f32, axis=-1, keepdims=True)
    inv_std = lax.rsqrt(jnp.mean(centered * centered, axis=-1, keepdims=True) + LN_EPS)
    x_hat = centered * inv_std
    normed = (x_hat * ln_gamma + ln_beta).astype(jnp.bfloat16)
    w_flat = w_qkv.reshape(D, 3 * D)
    qkv_all = jnp.dot(normed, w_flat, preferred_element_type=jnp.float32).astype(jnp.bfloat16).reshape(TOKENS, 3, HEADS, HEAD)
    q_raw = qkv_all[:, 0].astype(jnp.float32)
    k_raw = qkv_all[:, 1].astype(jnp.float32)
    v_heads = qkv_all[:, 2].astype(jnp.float32)
    feat_q = phi_act(q_raw).astype(jnp.bfloat16).astype(jnp.float32)
    feat_k = phi_act(k_raw).astype(jnp.bfloat16).astype(jnp.float32)
    state_b = jnp.einsum("nhi,nhj->hij", feat_k, v_heads).astype(jnp.bfloat16).astype(jnp.float32)
    norm_b = jnp.sum(feat_k, axis=0).astype(jnp.bfloat16).astype(jnp.float32)
    numerator = jnp.einsum("nhi,hij->nhj", feat_q, state_b)
    denominator = jnp.einsum("nhi,hi->nh", feat_q, norm_b)
    att_f32 = numerator / denominator[:, :, None]
    att_out = att_f32.astype(jnp.bfloat16).reshape(TOKENS, D)
    y_tok = (x_f32 + jnp.dot(att_out, w_out, preferred_element_type=jnp.float32)).astype(jnp.bfloat16)
    dw_out = jnp.dot(att_out.T, dy_tok, preferred_element_type=jnp.float32)
    d_att = jnp.dot(dy_tok, w_out.T, preferred_element_type=jnp.float32).reshape(TOKENS, HEADS, HEAD)
    g_scaled = (d_att / denominator[:, :, None]).astype(jnp.bfloat16).astype(jnp.float32)
    correction = jnp.sum(g_scaled * att_f32, axis=-1)
    d_fq = jnp.einsum("nhj,hij->nhi", g_scaled, state_b) - correction[:, :, None] * norm_b
    d_state_b = jnp.einsum("nhi,nhj->hij", feat_q, g_scaled).astype(jnp.bfloat16).astype(jnp.float32)
    d_norm = -jnp.einsum("nh,nhi->hi", correction, feat_q)
    d_fk = jnp.einsum("nhj,hij->nhi", v_heads, d_state_b) + d_norm
    d_val = jnp.einsum("nhi,hij->nhj", feat_k, d_state_b)
    d_q = (d_fq * phi_slope(q_raw)).astype(jnp.bfloat16)
    d_k = (d_fk * phi_slope(k_raw)).astype(jnp.bfloat16)
    d_qkv = jnp.stack([d_q, d_k, d_val.astype(jnp.bfloat16)], axis=1).reshape(TOKENS, 3 * D)
    dw_qkv = jnp.dot(normed.T, d_qkv, preferred_element_type=jnp.float32).reshape(D, 3, HEADS, HEAD)
    d_normed = jnp.dot(d_qkv, w_flat.T, preferred_element_type=jnp.float32)
    d_gamma = jnp.sum(d_normed * x_hat, axis=0)
    d_beta = jnp.sum(d_normed, axis=0)
    scaled_grad = d_normed * ln_gamma
    d_ln = inv_std * (scaled_grad - jnp.mean(scaled_grad, axis=-1, keepdims=True) - x_hat * jnp.mean(scaled_grad * x_hat, axis=-1, keepdims=True))
    dx_tok = (dy_tok.astype(jnp.float32) + d_ln).astype(jnp.bfloat16)
    return (y_tok, dx_tok, dw_qkv, dw_out, d_gamma, d_beta)
```

```python
import functools

import jax
import jax.numpy as jnp
from jax import lax
from jax.experimental import pallas as pl
from jax.experimental.pallas import tpu as pltpu
from jax.sharding import PartitionSpec as P

LN_EPS = 1e-5
MESH = pl.DeviceIdType.MESH
F32 = jnp.float32
BF16 = jnp.bfloat16
TT = 512
BLK = 256


def nn(a, b):
    return lax.dot_general(a, b, (((1,), (0,)), ((), ())), preferred_element_type=F32)


def nt(a, b):
    return lax.dot_general(a, b, (((1,), (1,)), ((), ())), preferred_element_type=F32)


def kernel(n, heads, hd,
           x_hbm, dy_hbm, gam_ref, bet_ref, wt_hbm, wo_hbm,
           y_hbm, dx_hbm, dwqkv_ref, dwo_ref, dg_ref, db_ref,
           xbuf, dybuf, wt, wo, w, wot, xT, dyT, uT, qkvT, oT, mean_ref, rstd_ref, gb, bb,
           s_acc, comp, ar_in, ar_out, sx, sg, sgt, zb, dzacc,
           acc, d2d, relay, fin, dgacc, dbacc, dgslots,
           sem_in, sem_out, ar_send, ar_recv, rs_send, rs_recv, dg_send, dg_recv):
    tokens, width = xbuf.shape
    steps = tokens // TT
    groups = 4
    hpg = heads // groups
    gr = hpg * hd
    nb = width // BLK
    chips = n // 2
    me = lax.axis_index("seq")
    chip, core = lax.div(me, 2), lax.rem(me, 2)
    partner = 2 * chip + (1 - core)
    c_right, c_left = lax.rem(chip + 1, chips), lax.rem(chip + chips - 1, chips)
    c_opp = lax.rem(chip + 2, chips)
    right, left = 2 * c_right + core, 2 * c_left + core

    def x_copy(t):
        r = pl.ds(pl.multiple_of(t * TT, TT), TT)
        return pltpu.make_async_copy(x_hbm.at[r, :], xbuf.at[r, :], sem_in.at[0, t])

    def dy_copy(t):
        r = pl.ds(pl.multiple_of(t * TT, TT), TT)
        return pltpu.make_async_copy(dy_hbm.at[r, :], dybuf.at[r, :], sem_in.at[1, t])

    wkv_copy = pltpu.make_async_copy(wt_hbm.at[pl.ds(width, 2 * width), :], wt.at[pl.ds(width, 2 * width), :], sem_in.at[2, 0])
    wq_copy = pltpu.make_async_copy(wt_hbm.at[pl.ds(0, width), :], wt.at[pl.ds(0, width), :], sem_in.at[2, 1])
    wo_copy = pltpu.make_async_copy(wo_hbm, wo, sem_in.at[2, 2])
    x_copy(0).start()
    wkv_copy.start()
    for t in range(1, steps):
        x_copy(t).start()
    for t in range(steps):
        dy_copy(t).start()
    wq_copy.start()
    wo_copy.start()

    barrier = pltpu.get_barrier_semaphore()
    for d in range(1, n):
        pl.semaphore_signal(barrier, inc=1, device_id={"seq": lax.rem(me + d, n)}, device_id_type=MESH)

    eye = (lax.broadcasted_iota(jnp.int32, (BLK, BLK), 0) == lax.broadcasted_iota(jnp.int32, (BLK, BLK), 1)).astype(F32).astype(BF16)
    gb[...] = jnp.transpose(jnp.broadcast_to(gam_ref[...], (128, width)))
    bb[...] = jnp.transpose(jnp.broadcast_to(bet_ref[...], (128, width)))
    s_acc[...] = jnp.zeros_like(s_acc)
    sx[...] = jnp.zeros_like(sx)
    dzacc[...] = jnp.zeros_like(dzacc)
    dgacc[...] = jnp.zeros_like(dgacc)
    dbacc[...] = jnp.zeros_like(dbacc)

    def lanes(ref_val):
        return jnp.concatenate([ref_val] * (TT // 128), axis=1)

    def fold(v):
        out = v[:, :128]
        for i in range(1, TT // 128):
            out = out + v[:, 128 * i:128 * (i + 1)]
        return out

    def tok(t):
        return pl.ds(pl.multiple_of(t * TT, TT), TT)

    wkv_copy.wait()

    @pl.loop(0, steps)
    def _(t):
        ts = tok(t)
        x_copy(t).wait()
        xt = jnp.concatenate([nt(eye, xbuf[ts, BLK * b:BLK * (b + 1)]) for b in range(nb)], axis=0)
        xT[:, ts] = xt.astype(BF16)
        mean = jnp.sum(xt, axis=0, keepdims=True) * (1.0 / width)
        cen = xt - mean
        var = jnp.sum(cen * cen, axis=0, keepdims=True) * (1.0 / width)
        rstd = lax.rsqrt(var + LN_EPS)
        mean_ref[:, ts] = mean
        rstd_ref[:, ts] = rstd
        uT[:, ts] = (cen * rstd * lanes(gb[...]) + lanes(bb[...])).astype(BF16)
        for g in range(groups):
            ks, vs = width + gr * g, 2 * width + gr * g
            kb = nn(wt[ks:ks + gr, :], uT[:, ts]).astype(BF16)
            vb = nn(wt[vs:vs + gr, :], uT[:, ts]).astype(BF16)
            qkvT[ks:ks + gr, ts] = kb
            qkvT[vs:vs + gr, ts] = vb
            k32 = kb.astype(F32)
            fk = jnp.where(k32 > 0, k32 + 1.0, jnp.exp(jnp.minimum(k32, 0.0))).astype(BF16)
            ve = jnp.concatenate([vb, jnp.ones((BLK - gr, TT), BF16)], axis=0)
            s_acc[g] += nt(fk, ve)

    lane128 = lax.broadcasted_iota(jnp.int32, (hd, 128), 1)
    lane256 = lax.broadcasted_iota(jnp.int32, (hd, BLK), 1)
    half_heads = heads // 2

    def compact(z_of):
        def head(h):
            g, hh = h // hpg, h % hpg
            blk = s_acc[g, hd * hh:hd * (hh + 1), :]
            moved = pltpu.roll(blk, BLK - hd * hh, axis=1) if hh else blk
            return jnp.where(lane128 < hd, moved[:, :128], jnp.where(lane128 == hd, z_of(h, blk), 0.0))

        for p in range(half_heads):
            comp[p] = head(p) + pltpu.roll(head(p + half_heads), 64, axis=1)

    def ar1(i, d):
        peer = lax.rem(me + d, n)
        return pltpu.make_async_remote_copy(
            src_ref=comp.at[peer], dst_ref=ar_in.at[i, d], send_sem=ar_send.at[2 * i, d], recv_sem=ar_recv.at[2 * i, d],
            device_id={"seq": peer}, device_id_type=MESH)

    def ar2(i, d):
        peer = lax.rem(me + d, n)
        return pltpu.make_async_remote_copy(
            src_ref=ar_out.at[i, 0], dst_ref=ar_out.at[i, d], send_sem=ar_send.at[2 * i + 1, d], recv_sem=ar_recv.at[2 * i + 1, d],
            device_id={"seq": peer}, device_id_type=MESH)

    def ar_reduce(i):
        total = comp[me]
        for d in range(1, n):
            ar1(i, d).wait_recv()
            total = total + ar_in[i, d]
        ar_out[i, 0] = total
        for d in range(1, n):
            ar1(i, d).wait_send()
        for d in range(1, n):
            ar2(i, d).start()

    def ar_finish(i, z_round, with_z):
        for d in range(1, n):
            ar2(i, d).wait_recv()
        for p in range(half_heads):
            piece = ar_out[i, lax.rem(me - p + n, n)]
            for h, part in ((p, piece), (p + half_heads, pltpu.roll(piece, 64, axis=1))):
                g, hh = h // hpg, h % hpg
                zc = part[:, hd:hd + 1]
                if z_round:
                    zc = zc.astype(BF16).astype(F32)
                blk = jnp.where(lane128 < hd, part, 0.0)
                wide = jnp.concatenate([blk, jnp.zeros((hd, 128), F32)], axis=1)
                if hh:
                    wide = pltpu.roll(wide, hd * hh, axis=1)
                if with_z:
                    wide = jnp.where(lane256 == gr + hh, jnp.broadcast_to(zc, (hd, BLK)), wide)
                sx[g, hd * hh:hd * (hh + 1), :] = wide
                zb[hd * h:hd * (h + 1), :] = jnp.broadcast_to(zc, (hd, 128))
        for g in range(groups):
            m = sx[g]
            sg[g] = m[:gr, :gr].astype(BF16)
            sgt[g] = jnp.transpose(m)[:sgt.shape[1], :gr].astype(BF16)

    compact(lambda h, blk: blk[:, gr:gr + 1])
    pl.semaphore_wait(barrier, n - 1)
    for d in range(1, n):
        ar1(0, d).start()

    wq_copy.wait()

    @pl.loop(0, steps)
    def _(t):
        ts = tok(t)
        dy_copy(t).wait()
        for b in range(nb):
            dyT[BLK * b:BLK * (b + 1), ts] = nt(eye, dybuf[ts, BLK * b:BLK * (b + 1)]).astype(BF16)
        qkvT[0:width, ts] = nn(wt[0:width, :], uT[:, ts]).astype(BF16)

    ar_reduce(0)
    wo_copy.wait()
    for i in range(nb):
        for j in range(nb):
            wot[BLK * j:BLK * (j + 1), BLK * i:BLK * (i + 1)] = nt(eye, wo[BLK * i:BLK * (i + 1), BLK * j:BLK * (j + 1)]).astype(BF16)

    @pl.loop(0, 3 * nb)
    def _(j):
        js = pl.ds(pl.multiple_of(j * BLK, BLK), BLK)
        for i in range(nb):
            w[BLK * i:BLK * (i + 1), js] = nt(eye, wt[js, BLK * i:BLK * (i + 1)]).astype(BF16)

    ar_finish(0, True, True)
    s_acc[...] = jnp.zeros_like(s_acc)

    def per_head(v):
        return jnp.broadcast_to(v[:, None, :], (hpg, hd, TT)).reshape(gr, TT)

    @pl.loop(0, steps)
    def _(t):
        ts = tok(t)
        for g in range(groups):
            rows = slice(gr * g, gr * (g + 1))
            q32 = qkvT[rows, ts].astype(F32)
            ex = jnp.exp(jnp.minimum(q32, 0.0))
            fq = jnp.where(q32 > 0, q32 + 1.0, ex).astype(BF16)
            slope = jnp.where(q32 > 0, 1.0, ex)
            nd = nn(sgt[g], fq)
            rden = per_head(1.0 / nd[gr:gr + hpg])
            a = nd[:gr] * rden
            oT[rows, ts] = a.astype(BF16)
            gg = (nn(wo[rows, :], dyT[:, ts]) * rden).astype(BF16)
            c = jnp.sum((gg.astype(F32) * a).reshape(hpg, hd, TT), axis=1)
            cb = per_head(c)
            dfq = nn(sg[g], gg) - cb * lanes(zb[rows, :])
            qkvT[rows, ts] = (dfq * slope).astype(BF16)
            ge = jnp.concatenate([gg, jnp.zeros((BLK - gr, TT), BF16)], axis=0)
            s_acc[g] += nt(fq, ge)
            dzacc[rows, :] -= fold(cb * fq.astype(F32))

    compact(lambda h, blk: jnp.sum(dzacc[hd * h:hd * (h + 1), :], axis=1, keepdims=True))
    for d in range(1, n):
        ar1(1, d).start()

    half_rows = width // 2

    def grad_wo():
        @pl.loop(0, 2)
        def _(m):
            rs = pl.ds(pl.multiple_of(m * half_rows, half_rows), half_rows)
            out = nn(oT[rs, :], dybuf[...])
            acc[0, pl.ds(2 * m, 2)] = out.reshape(2, 2, width // n, width)

    def grad_w(j):
        @pl.loop(0, 2)
        def _(m):
            rs = pl.ds(pl.multiple_of(m * half_rows, half_rows), half_rows)
            out = nt(uT[rs, :], qkvT[width * (j - 1):width * j, :])
            acc[j, pl.ds(2 * m, 2)] = out.reshape(2, 2, width // n, width)

    hr = width // n // 2
    lo, hi = pl.ds(0, hr), pl.ds(hr, hr)

    def rdma(u, s, src, dst, peer):
        return pltpu.make_async_remote_copy(src_ref=src, dst_ref=dst, send_sem=rs_send.at[u, s], recv_sem=rs_recv.at[u, s],
                                            device_id={"seq": peer}, device_id_type=MESH)

    def d2d_copy(u, c):
        return rdma(u, c, acc.at[u, c, 1 - core], d2d.at[u, c], partner)

    def hop(u, s):
        if s == 0:
            return rdma(u, chips, acc.at[u, c_opp, core, lo], relay.at[u, 0], right)
        if s == 1:
            return rdma(u, chips + 1, acc.at[u, c_opp, core, hi], relay.at[u, 1], left)
        if s == 2:
            return rdma(u, chips + 2, acc.at[u, c_right, core, hi], fin.at[u, 0, hi], right)
        if s == 3:
            return rdma(u, chips + 3, acc.at[u, c_left, core, lo], fin.at[u, 1, lo], left)
        if s == 4:
            return rdma(u, chips + 4, acc.at[u, c_right, core, lo], fin.at[u, 0, lo], right)
        return rdma(u, chips + 5, acc.at[u, c_left, core, hi], fin.at[u, 1, hi], left)

    def rs_pair(u):
        for c in range(chips):
            d2d_copy(u, c).start()

    def rs_chip(u):
        for c in range(chips):
            d2d_copy(u, c).wait_recv()
        acc[u, c_opp, core] += d2d[u, c_opp]
        hop(u, 0).start()
        hop(u, 1).start()
        acc[u, c_right, core] += d2d[u, c_right]
        hop(u, 2).start()
        acc[u, c_left, core] += d2d[u, c_left]
        hop(u, 3).start()
        acc[u, chip, core] += d2d[u, chip]

    def rs_relay(u):
        hop(u, 0).wait_recv()
        acc[u, c_right, core, lo] += relay[u, 0]
        hop(u, 4).start()
        hop(u, 1).wait_recv()
        acc[u, c_left, core, hi] += relay[u, 1]
        hop(u, 5).start()

    def rs_final(u, out_ref, cols):
        for s in range(2, 6):
            hop(u, s).wait_recv()
        out_ref[:, cols] = acc[u, chip, core] + fin[u, 0] + fin[u, 1]

    grad_wo()
    rs_pair(0)
    ar_reduce(1)
    grad_w(1)
    rs_pair(1)
    rs_chip(0)
    ar_finish(1, False, False)

    @pl.loop(0, steps)
    def _(t):
        ts = tok(t)
        for g in range(groups):
            kr = slice(width + gr * g, width + gr * (g + 1))
            vr = slice(2 * width + gr * g, 2 * width + gr * (g + 1))
            k32 = qkvT[kr, ts].astype(F32)
            ex = jnp.exp(jnp.minimum(k32, 0.0))
            fk = jnp.where(k32 > 0, k32 + 1.0, ex).astype(BF16)
            slope = jnp.where(k32 > 0, 1.0, ex)
            dfk = nn(sg[g], qkvT[vr, ts]) + lanes(zb[gr * g:gr * (g + 1), :])
            qkvT[kr, ts] = (dfk * slope).astype(BF16)
            qkvT[vr, ts] = nn(sgt[g, :gr, :], fk).astype(BF16)

    rs_chip(1)
    grad_w(2)
    rs_pair(2)
    rs_relay(0)
    grad_w(3)
    rs_pair(3)
    rs_chip(2)
    rs_relay(1)

    def y_copy(t):
        r = tok(t)
        return pltpu.make_async_copy(xbuf.at[r, :], y_hbm.at[r, :], sem_out.at[0, t])

    def dx_copy(t):
        r = tok(t)
        return pltpu.make_async_copy(dybuf.at[r, :], dx_hbm.at[r, :], sem_out.at[1, t])

    def store_tokens(buf, t, val):
        for s in range(TT // BLK):
            r = pl.ds(pl.multiple_of(t * TT + BLK * s, BLK), BLK)
            for b in range(nb):
                buf[r, BLK * b:BLK * (b + 1)] = nt(eye, val[BLK * b:BLK * (b + 1), BLK * s:BLK * (s + 1)]).astype(BF16)

    @pl.loop(0, steps)
    def _(t):
        ts = tok(t)
        yt = (nn(wot[...], oT[:, ts]) + xT[:, ts].astype(F32)).astype(BF16)
        store_tokens(xbuf, t, yt)
        y_copy(t).start()

    rs_chip(3)

    @pl.loop(0, steps)
    def _(t):
        ts = tok(t)
        du = nn(w[...], qkvT[:, ts])
        rstd = rstd_ref[:, ts]
        xhat = (xT[:, ts].astype(F32) - mean_ref[:, ts]) * rstd
        dgacc[...] += fold(du * xhat)
        dbacc[...] += fold(du)
        e = du * lanes(gb[...])
        m1 = jnp.sum(e, axis=0, keepdims=True) * (1.0 / width)
        m2 = jnp.sum(e * xhat, axis=0, keepdims=True) * (1.0 / width)
        dxt = (dyT[:, ts].astype(F32) + rstd * (e - m1 - xhat * m2)).astype(BF16)
        store_tokens(dybuf, t, dxt)
        dx_copy(t).start()

    def dg_copy(d):
        return pltpu.make_async_remote_copy(
            src_ref=dgslots.at[0], dst_ref=dgslots.at[d], send_sem=dg_send.at[d], recv_sem=dg_recv.at[d],
            device_id={"seq": lax.rem(me + d, n)}, device_id_type=MESH)

    dgrow = jnp.sum(jnp.transpose(dgacc[...]), axis=0, keepdims=True)
    dbrow = jnp.sum(jnp.transpose(dbacc[...]), axis=0, keepdims=True)
    sub = lax.broadcasted_iota(jnp.int32, (8, width), 0)
    dgslots[0] = jnp.where(sub == 0, dgrow, jnp.where(sub == 1, dbrow, 0.0))
    for d in range(1, n):
        dg_copy(d).start()

    rs_relay(2)
    rs_relay(3)
    rs_final(0, dwo_ref, slice(0, width))
    for u in range(1, 4):
        rs_final(u, dwqkv_ref, slice(width * (u - 1), width * u))

    for d in range(1, n):
        dg_copy(d).wait_recv()
    total = dgslots[lax.rem(me, n)]
    for p in range(1, n):
        total = total + dgslots[lax.rem(me - p + n, n)]
    dg_ref[...] = total[0:1]
    db_ref[...] = total[1:2]

    for d in range(1, n):
        ar2(0, d).wait_send()
        ar2(1, d).wait_send()
        dg_copy(d).wait_send()
    for u in range(4):
        for c in range(chips):
            d2d_copy(u, c).wait_send()
        for s in range(6):
            hop(u, s).wait_send()

    @pl.loop(0, steps)
    def _(t):
        y_copy(t).wait()
        dx_copy(t).wait()


def local_block(n, x_tok, dy_tok, ln_gamma, ln_beta, w_qkv, w_out):
    tokens, width = x_tok.shape
    _, three, heads, hd = w_qkv.shape
    wt = w_qkv.transpose(1, 2, 3, 0).reshape(three * width, width)
    steps = tokens // TT
    chips = n // 2
    own = width // n
    hbm = pl.BlockSpec(memory_space=pl.ANY)
    vmem = pl.BlockSpec(memory_space=pltpu.VMEM)
    gr = heads * hd // 4
    dma = pltpu.SemaphoreType.DMA
    y, dx, dwqkv, dwo, dg, db = pl.pallas_call(
        functools.partial(kernel, n, heads, hd),
        name="block",
        out_shape=(
            jax.ShapeDtypeStruct((tokens, width), BF16), jax.ShapeDtypeStruct((tokens, width), BF16),
            jax.ShapeDtypeStruct((own, three * width), F32), jax.ShapeDtypeStruct((own, width), F32),
            jax.ShapeDtypeStruct((1, width), F32), jax.ShapeDtypeStruct((1, width), F32)),
        in_specs=[hbm, hbm, vmem, vmem, hbm, hbm],
        out_specs=(hbm, hbm, vmem, vmem, vmem, vmem),
        scratch_shapes=[
            pltpu.VMEM((tokens, width), BF16), pltpu.VMEM((tokens, width), BF16),
            pltpu.VMEM((three * width, width), BF16), pltpu.VMEM((width, width), BF16),
            pltpu.VMEM((width, three * width), BF16), pltpu.VMEM((width, width), BF16),
            pltpu.VMEM((width, tokens), BF16), pltpu.VMEM((width, tokens), BF16), pltpu.VMEM((width, tokens), BF16),
            pltpu.VMEM((three * width, tokens), BF16), pltpu.VMEM((width, tokens), BF16),
            pltpu.VMEM((1, tokens), F32), pltpu.VMEM((1, tokens), F32),
            pltpu.VMEM((width, 128), F32), pltpu.VMEM((width, 128), F32),
            pltpu.VMEM((4, gr, BLK), F32), pltpu.VMEM((heads // 2, hd, 128), F32),
            pltpu.VMEM((2, n, hd, 128), F32), pltpu.VMEM((2, n, hd, 128), F32),
            pltpu.VMEM((4, BLK, BLK), F32), pltpu.VMEM((4, gr, gr), BF16), pltpu.VMEM((4, gr + 16, gr), BF16),
            pltpu.VMEM((width, 128), F32), pltpu.VMEM((width, 128), F32),
            pltpu.VMEM((4, chips, 2, own, width), F32), pltpu.VMEM((4, chips, own, width), F32),
            pltpu.VMEM((4, 2, own // 2, width), F32), pltpu.VMEM((4, 2, own, width), F32),
            pltpu.VMEM((width, 128), F32), pltpu.VMEM((width, 128), F32), pltpu.VMEM((n, 8, width), F32),
            dma((3, max(steps, 3))), dma((2, steps)),
            dma((4, n)), dma((4, n)), dma((4, chips + 6)), dma((4, chips + 6)), dma((n,)), dma((n,)),
        ],
        compiler_params=pltpu.CompilerParams(collective_id=0, has_side_effects=True, vmem_limit_bytes=67_000_000),
    )(x_tok, dy_tok, ln_gamma.reshape(1, width), ln_beta.reshape(1, width), wt, w_out)
    return y, dx, dwqkv.reshape(own, three, heads, hd), dwo, dg.reshape(width), db.reshape(width)


def solution(mesh):
    rows = P(("data", "seq"), None)
    return jax.shard_map(
        functools.partial(local_block, mesh.shape["seq"]), mesh=mesh,
        in_specs=(rows, rows, P(None), P(None), P(None, None, None, None), P(None, None)),
        out_specs=(rows, rows, P(("data", "seq"), None, None, None), rows, P("data"), P("data")),
        check_vma=False)
```

```python
import functools

import jax
import jax.numpy as jnp
from jax import lax
from jax.experimental import pallas as pl
from jax.experimental.pallas import tpu as pltpu
from jax.sharding import PartitionSpec as P

LN_EPS = 1e-5
MESH = pl.DeviceIdType.MESH
F32 = jnp.float32
BF16 = jnp.bfloat16
TT = 512
BLK = 256


def nn(a, b):
    return lax.dot_general(a, b, (((1,), (0,)), ((), ())), preferred_element_type=F32)


def nt(a, b):
    return lax.dot_general(a, b, (((1,), (1,)), ((), ())), preferred_element_type=F32)


def kernel(n, heads, hd,
           x_hbm, dy_hbm, gam_ref, bet_ref, wt_hbm, wo_hbm,
           y_hbm, dx_hbm, dwqkv_hbm, dwo_hbm, dg_ref, db_ref,
           xbuf, dybuf, wt, wo, w, xT, dyT, uT, qkvT, oT, mean_ref, rstd_ref, gb, bb,
           s_acc, comp, ar_in, ar_out, sx, sg, sgt, ubuf,
           acc, d2d, relay, fin, dgacc, dbacc, dgslots,
           sem_in, sem_out, ar_send, ar_recv, rs_send, rs_recv, dg_send, dg_recv):
    tokens, width = xbuf.shape
    steps = tokens // TT
    groups = 4
    hpg = heads // groups
    gr = hpg * hd
    nb = width // BLK
    chips = n // 2
    me = lax.axis_index("seq")
    chip, core = lax.div(me, 2), lax.rem(me, 2)
    partner = 2 * chip + (1 - core)
    c_right, c_left = lax.rem(chip + 1, chips), lax.rem(chip + chips - 1, chips)
    c_opp = lax.rem(chip + 2, chips)
    right, left = 2 * c_right + core, 2 * c_left + core

    def x_copy(t):
        r = pl.ds(pl.multiple_of(t * TT, TT), TT)
        return pltpu.make_async_copy(x_hbm.at[r, :], xbuf.at[r, :], sem_in.at[0, t])

    def dy_copy(t):
        r = pl.ds(pl.multiple_of(t * TT, TT), TT)
        return pltpu.make_async_copy(dy_hbm.at[r, :], dybuf.at[r, :], sem_in.at[1, t])

    wkv_copy = pltpu.make_async_copy(wt_hbm.at[pl.ds(width, 2 * width), :], wt.at[pl.ds(width, 2 * width), :], sem_in.at[2, 0])
    wq_copy = pltpu.make_async_copy(wt_hbm.at[pl.ds(0, width), :], wt.at[pl.ds(0, width), :], sem_in.at[2, 1])
    wo_copy = pltpu.make_async_copy(wo_hbm, wo, sem_in.at[2, 2])
    x_copy(0).start()
    wkv_copy.start()
    for t in range(1, steps):
        x_copy(t).start()
    for t in range(steps):
        dy_copy(t).start()
    wq_copy.start()
    wo_copy.start()

    barrier = pltpu.get_barrier_semaphore()
    for d in range(1, n):
        pl.semaphore_signal(barrier, inc=1, device_id={"seq": lax.rem(me + d, n)}, device_id_type=MESH)

    eye = (lax.broadcasted_iota(jnp.int32, (BLK, BLK), 0) == lax.broadcasted_iota(jnp.int32, (BLK, BLK), 1)).astype(F32).astype(BF16)
    gb[...] = jnp.transpose(jnp.broadcast_to(gam_ref[...][None, :], (128, width)))
    bb[...] = jnp.transpose(jnp.broadcast_to(bet_ref[...][None, :], (128, width)))
    s_acc[...] = jnp.zeros_like(s_acc)
    sx[...] = jnp.zeros_like(sx)
    dgacc[...] = jnp.zeros_like(dgacc)
    dbacc[...] = jnp.zeros_like(dbacc)

    def lanes(ref_val, tt=TT):
        return jnp.concatenate([ref_val] * (tt // 128), axis=1)

    def fold(v):
        out = v[:, :128]
        for i in range(1, TT // 128):
            out = out + v[:, 128 * i:128 * (i + 1)]
        return out

    def tok(t, tt=TT):
        return pl.ds(t * tt if isinstance(t, int) else pl.multiple_of(t * tt, tt), tt)

    def phi(v32):
        ex = jnp.exp(jnp.minimum(v32, 0.0))
        pos = v32 > 0
        return jnp.where(pos, v32 + 1.0, ex).astype(BF16), jnp.where(pos, 1.0, ex)

    def parts3(v):
        p1 = v.astype(BF16).astype(F32)
        r = v - p1
        p2 = r.astype(BF16).astype(F32)
        return p1, p2, (r - p2).astype(BF16).astype(F32)

    scope = jax.named_scope
    ones_rows = jnp.ones((BLK - gr, TT), BF16)

    def norm_tile(t):
        ts = tok(t)
        xt = jnp.concatenate([nt(eye, xbuf[ts, BLK * b:BLK * (b + 1)]) for b in range(nb)], axis=0)
        xT[:, ts] = xt.astype(BF16)
        mean = jnp.sum(xt, axis=0, keepdims=True) * (1.0 / width)
        cen = xt - mean
        var = jnp.sum(cen * cen, axis=0, keepdims=True) * (1.0 / width)
        rstd = lax.rsqrt(var + LN_EPS)
        mean_ref[:, ts] = mean
        rstd_ref[:, ts] = rstd
        u = (cen * rstd * lanes(gb[...]) + lanes(bb[...])).astype(BF16)
        uT[:, ts] = u
        ubuf[t % 2] = u

    def kv_mm(t, half, u):
        ts = tok(t)
        hw = width // 2
        kb = nn(wt[width + hw * half:width + hw * (half + 1), :], u[...]).astype(BF16)
        vb = nn(wt[2 * width + hw * half:2 * width + hw * (half + 1), :], u[...]).astype(BF16)
        qkvT[width + hw * half:width + hw * (half + 1), ts] = kb
        qkvT[2 * width + hw * half:2 * width + hw * (half + 1), ts] = vb
        return half, phi(kb.astype(F32))[0], vb

    def s_mm(half, fk, vb):
        for i, g in enumerate(half_groups(half)):
            rows = slice(gr * i, gr * (i + 1))
            s_acc[g] += nt(fk[rows], jnp.concatenate([vb[rows], ones_rows], axis=0))

    def half_groups(half):
        return range(groups // 2 * half, groups // 2 * (half + 1))

    lane128 = lax.broadcasted_iota(jnp.int32, (hd, 128), 1)
    lane256 = lax.broadcasted_iota(jnp.int32, (hd, BLK), 1)
    lane_sx = lax.broadcasted_iota(jnp.int32, (BLK, BLK), 1)
    rows_owned = hd // 2

    def compact(e, z_of):
        g0 = groups // 2 * (e % 2)

        def head(g, hh):
            blk = s_acc[g, hd * hh:hd * (hh + 1), :]
            moved = pltpu.roll(blk, BLK - hd * hh, axis=1) if hh else blk
            return jnp.where(lane128 < hd, moved[:, :128], jnp.where(lane128 == hd, z_of(hh, blk), 0.0))

        for j in range(hpg):
            pair = head(g0, j) + pltpu.roll(head(g0 + 1, j), 64, axis=1)
            comp[e, 2 * j] = pair[:rows_owned]
            comp[e, 2 * j + 1] = pair[rows_owned:]
        s_acc[g0:g0 + 2] = jnp.zeros((2, gr, BLK), F32)
        for d in range(1, n):
            ar1(e, d).start()

    def ar1(e, d):
        peer = lax.rem(me + d, n)
        return pltpu.make_async_remote_copy(
            src_ref=comp.at[e, peer], dst_ref=ar_in.at[e, d], send_sem=ar_send.at[2 * e, d], recv_sem=ar_recv.at[2 * e, d],
            device_id={"seq": peer}, device_id_type=MESH)

    def ar2(e, d):
        peer = lax.rem(me + d, n)
        return pltpu.make_async_remote_copy(
            src_ref=ar_out.at[e, 0], dst_ref=ar_out.at[e, d], send_sem=ar_send.at[2 * e + 1, d], recv_sem=ar_recv.at[2 * e + 1, d],
            device_id={"seq": peer}, device_id_type=MESH)

    def ar_reduce(i):
        total = comp[i, me]
        for d in range(1, n):
            ar1(i, d).wait_recv()
            total = total + ar_in[i, d]
        ar_out[i, 0] = total
        for d in range(1, n):
            ar2(i, d).start()

    def ar_finish(i):
        forward = i < 2
        for d in range(1, n):
            ar2(i, d).wait_recv()
        for g in half_groups(i % 2):
            for hh in range(hpg):
                part = jnp.concatenate([ar_out[i, lax.rem(me - p + n, n)] for p in (2 * hh, 2 * hh + 1)], axis=0)
                if g % 2:
                    part = pltpu.roll(part, 64, axis=1)
                wide = jnp.concatenate([jnp.where(lane128 < hd, part, 0.0), jnp.zeros((hd, 128), F32)], axis=1)
                if hh:
                    wide = pltpu.roll(wide, hd * hh, axis=1)
                zc = part[:, hd:hd + 1]
                if forward:
                    hit = (lane256 == gr + hh) | (lane256 == gr + hpg + hh) | (lane256 == gr + 2 * hpg + hh)
                    wide = jnp.where(hit, jnp.broadcast_to(zc, (hd, BLK)), wide)
                else:
                    for j, zp in enumerate(parts3(jnp.broadcast_to(zc, (hd, BLK)))):
                        wide = jnp.where(lane256 == gr + j, zp, wide)
                sx[hd * hh:hd * (hh + 1), :] = wide
            m = sx[...]
            ext = jnp.where(lane_sx >= gr, -m, m) if forward else m
            sg[g] = ext[:gr, :gr + 16].astype(BF16)
            sgt[g] = jnp.transpose(m)[:gr + 16, :gr].astype(BF16)

    def z_fwd(hh, blk):
        return blk[:, gr:gr + 1]

    off = lane128 - (gr - 128)

    def z_bwd(hh, blk):
        hit = (off >= 0) & (off < 3 * hpg) & (lax.rem(off, hpg) == hh)
        return -jnp.sum(jnp.where(hit, blk[:, 128:], 0.0), axis=1, keepdims=True)

    def do_half(half):
        @pl.loop(0, steps)
        def _(t):
            hw = width // 2
            acc[t, pl.ds(2 * half, 2), :, :, :TT] = nn(wo[hw * half:hw * (half + 1), :], dyT[:, tok(t)]).reshape(2, 2, gr // 2, TT)

    def q_tile(t):
        ts = tok(t)
        dy_copy(t).wait()
        for b in range(nb):
            dyT[BLK * b:BLK * (b + 1), ts] = nt(eye, dybuf[ts, BLK * b:BLK * (b + 1)]).astype(BF16)
        qkvT[0:width, ts] = nn(wt[0:width, :], uT[:, ts]).astype(BF16)

    with scope("A0"):
        x_copy(0).wait()
        norm_tile(0)
    wkv_copy.wait()
    for t in range(steps):
        with scope(f"A_{t}"):
            if t + 1 < steps:
                x_copy(t + 1).wait()
                norm_tile(t + 1)
            now = kv_mm(t, 0, ubuf.at[t % 2])
            if t:
                s_mm(*last)
            last = now
    with scope("A_s"):
        s_mm(*last)
    pl.semaphore_wait(barrier, n - 1)
    with scope("compact0"):
        compact(0, z_fwd)
    with scope("A2"):
        @pl.loop(0, steps)
        def _(t):
            s_mm(*kv_mm(t, 1, uT.at[:, tok(t)]))
    with scope("compact1"):
        compact(1, z_fwd)

    wq_copy.wait()
    with scope("fill_q0"):
        pl.loop(0, steps // 2)(q_tile)
    with scope("ar_reduce0"):
        ar_reduce(0)
    with scope("fill_q1"):
        pl.loop(steps // 2, steps)(q_tile)
    wo_copy.wait()
    with scope("do0"):
        do_half(0)
    with scope("ar_reduce1"):
        ar_reduce(1)
    with scope("ar_finish0"):
        ar_finish(0)

    def per_head(v):
        return jnp.broadcast_to(v[:, None, :], (hpg, hd, TT)).reshape(gr, TT)

    def b_tiles(i, half):
        pairs = [(i, g) for g in half_groups(half)]
        rows = {g: slice(gr * g, gr * (g + 1)) for _, g in pairs}
        feats = [phi(qkvT[rows[g], tok(t)].astype(F32)) for t, g in pairs]
        nds = [nn(sgt[g], fq) for (t, g), (fq, _) in zip(pairs, feats)]
        ges = []
        for (t, g), nd in zip(pairs, nds):
            rden = per_head(1.0 / nd[gr:gr + hpg])
            a = nd[:gr] * rden
            oT[rows[g], tok(t)] = a.astype(BF16)
            gg = (acc[t, g, :, :, :TT].reshape(gr, TT) * rden).astype(BF16)
            c = jnp.sum((gg.astype(F32) * a).reshape(hpg, hd, TT), axis=1)
            cp = jnp.concatenate(list(parts3(c)) + [jnp.zeros((hpg, TT), F32)], axis=0).astype(BF16)
            ges.append(jnp.concatenate([gg, cp], axis=0))
        dfqs = [nn(sg[g], ge) for (t, g), ge in zip(pairs, ges)]
        for (t, g), (fq, slope), ge, dfq in zip(pairs, feats, ges, dfqs):
            s_acc[g] += nt(fq, jnp.concatenate([ge, jnp.zeros((BLK - gr - 16, TT), BF16)], axis=0))
            qkvT[rows[g], tok(t)] = (dfq * slope).astype(BF16)

    own = width // n

    def grad(u):
        @pl.loop(0, 2)
        def _(m):
            half = lax.rem(lax.div(chip, 2) + 1 + m, 2)
            rs = pl.ds(pl.multiple_of(half * (width // 2), width // 2), width // 2)
            if u == 0:
                out = nn(oT[rs, :], dybuf[...])
            else:
                out = nt(uT[rs, :], qkvT[width * (u - 1):width * u, :])
            acc[u, pl.ds(2 * half, 2)] = out.reshape(2, 2, own, width)
            d2d_copy(u, 2 * half).start()
            d2d_copy(u, 2 * half + 1).start()

    hr = width // n // 2
    lo, hi = pl.ds(0, hr), pl.ds(hr, hr)

    def rdma(u, s, src, dst, peer):
        return pltpu.make_async_remote_copy(src_ref=src, dst_ref=dst, send_sem=rs_send.at[u, s], recv_sem=rs_recv.at[u, s],
                                            device_id={"seq": peer}, device_id_type=MESH)

    def d2d_copy(u, c):
        return rdma(u, c, acc.at[u, c, 1 - core], d2d.at[u, c], partner)

    def hop(u, s):
        if s == 0:
            return rdma(u, chips, acc.at[u, c_opp, core, lo], relay.at[u, 0], right)
        if s == 1:
            return rdma(u, chips + 1, acc.at[u, c_opp, core, hi], relay.at[u, 1], left)
        if s == 2:
            return rdma(u, chips + 2, acc.at[u, c_right, core, hi], fin.at[u, 0, hi], right)
        if s == 3:
            return rdma(u, chips + 3, acc.at[u, c_left, core, lo], fin.at[u, 1, lo], left)
        if s == 4:
            return rdma(u, chips + 4, acc.at[u, c_right, core, lo], fin.at[u, 0, lo], right)
        return rdma(u, chips + 5, acc.at[u, c_left, core, hi], fin.at[u, 1, hi], left)

    def rs_chip_a(u):
        d2d_copy(u, c_opp).wait_recv()
        acc[u, c_opp, core] += d2d[u, c_opp]
        hop(u, 0).start()
        hop(u, 1).start()

    def rs_chip_b(u):
        d2d_copy(u, c_right).wait_recv()
        acc[u, c_right, core] += d2d[u, c_right]
        hop(u, 2).start()
        d2d_copy(u, c_left).wait_recv()
        acc[u, c_left, core] += d2d[u, c_left]
        hop(u, 3).start()
        d2d_copy(u, chip).wait_recv()
        acc[u, chip, core] += d2d[u, chip]

    def rs_relay(u):
        hop(u, 0).wait_recv()
        acc[u, c_right, core, lo] += relay[u, 0]
        hop(u, 4).start()
        hop(u, 1).wait_recv()
        acc[u, c_left, core, hi] += relay[u, 1]
        hop(u, 5).start()

    def out_copy(u):
        dst = dwo_hbm if u == 0 else dwqkv_hbm.at[:, pl.ds(width * (u - 1), width)]
        return pltpu.make_async_copy(acc.at[u, chip, core], dst, sem_out.at[2, u])

    def rs_final(u):
        for s in range(2, 6):
            hop(u, s).wait_recv()
        acc[u, chip, core] += fin[u, 0] + fin[u, 1]
        out_copy(u).start()

    def y_copy(t):
        r = tok(t)
        return pltpu.make_async_copy(xbuf.at[r, :], y_hbm.at[r, :], sem_out.at[0, t])

    def dx_copy(t):
        r = tok(t)
        return pltpu.make_async_copy(dybuf.at[r, :], dx_hbm.at[r, :], sem_out.at[1, t])

    def store_tokens(buf, t, val):
        for s in range(TT // BLK):
            r = pl.ds(t * TT + BLK * s if isinstance(t, int) else pl.multiple_of(t * TT + BLK * s, BLK), BLK)
            for b in range(nb):
                buf[r, BLK * b:BLK * (b + 1)] = nt(eye, val[BLK * b:BLK * (b + 1), BLK * s:BLK * (s + 1)]).astype(BF16)

    def y_tile(t):
        ts = tok(t)
        yt = (nn(uT[:, 0:width], oT[:, ts]) + xT[:, ts].astype(F32)).astype(BF16)
        store_tokens(xbuf, t, yt)
        y_copy(t).start()

    def c_tiles(i, half):
        pairs = [(2 * i + k, g) for k in range(2) for g in half_groups(half)]
        krows = {g: slice(width + gr * g, width + gr * (g + 1)) for _, g in pairs}
        vrows = {g: slice(2 * width + gr * g, 2 * width + gr * (g + 1)) for _, g in pairs}
        dfks = [nn(sg[g], jnp.concatenate([qkvT[vrows[g], tok(t)], ones_rows[:16]], axis=0)) for t, g in pairs]
        feats = [phi(qkvT[krows[g], tok(t)].astype(F32)) for t, g in pairs]
        dvs = [nn(sgt[g, :gr, :], fk) for (t, g), (fk, _) in zip(pairs, feats)]
        for (t, g), (_, slope), dfk, dv in zip(pairs, feats, dfks, dvs):
            qkvT[krows[g], tok(t)] = (dfk * slope).astype(BF16)
            qkvT[vrows[g], tok(t)] = dv.astype(BF16)

    def du_tile(t):
        i = 2 * (t % 2)
        d2d[i:i + 2, :, :, :TT] = nn(w[...], qkvT[:, tok(t)]).reshape(2, chips, own, TT)

    def dx_tile(t):
        ts = tok(t)
        i = 2 * (t % 2)
        du = d2d[i:i + 2, :, :, :TT].reshape(width, TT)
        rstd = rstd_ref[:, ts]
        xhat = (xT[:, ts].astype(F32) - mean_ref[:, ts]) * rstd
        p = du * xhat
        dgacc[...] += fold(p)
        dbacc[...] += fold(du)
        gl = lanes(gb[...])
        e = du * gl
        m1 = jnp.sum(e, axis=0, keepdims=True) * (1.0 / width)
        m2 = jnp.sum(p * gl, axis=0, keepdims=True) * (1.0 / width)
        dxt = (dyT[:, ts].astype(F32) + rstd * (e - m1 - xhat * m2)).astype(BF16)
        store_tokens(dybuf, t, dxt)

    with scope("B0"):
        pl.loop(0, steps)(functools.partial(b_tiles, half=0))
    with scope("compact2"):
        compact(2, z_bwd)
    with scope("do1"):
        do_half(1)
    with scope("ar_finish1"):
        ar_finish(1)
    with scope("B1"):
        pl.loop(0, steps)(functools.partial(b_tiles, half=1))
    with scope("compact3"):
        compact(3, z_bwd)
    with scope("ar_reduce2"):
        ar_reduce(2)
    with scope("gradwo"):
        grad(0)
    with scope("rs_chip_a0"):
        rs_chip_a(0)
    with scope("ar_reduce3"):
        ar_reduce(3)
    with scope("rs_chip_b0"):
        rs_chip_b(0)
    with scope("gradwq"):
        grad(1)
    with scope("ar_finish2"):
        ar_finish(2)
    with scope("C0"):
        pl.loop(0, steps // 2)(functools.partial(c_tiles, half=0))
    with scope("ar_finish3"):
        ar_finish(3)
    with scope("relay0"):
        rs_relay(0)
        rs_chip_a(1)
    with scope("C1"):
        pl.loop(0, steps // 2)(functools.partial(c_tiles, half=1))
    with scope("rs_chip_b1"):
        rs_chip_b(1)
    with scope("gradwk"):
        grad(2)
    with scope("rs_chip_a2"):
        rs_chip_a(2)
        rs_chip_b(2)
    with scope("gradwv"):
        grad(3)
    with scope("relay1"):
        rs_relay(1)
    wot = uT.at[:, 0:width]
    with scope("fill_wo"):
        for i in range(nb):
            for j in range(nb):
                wot[BLK * j:BLK * (j + 1), BLK * i:BLK * (i + 1)] = nt(eye, wo[BLK * i:BLK * (i + 1), BLK * j:BLK * (j + 1)]).astype(BF16)
    with scope("fill_w"):
        @pl.loop(0, 3 * nb)
        def _(j):
            js = pl.ds(pl.multiple_of(j * BLK, BLK), BLK)
            for i in range(nb):
                w[BLK * i:BLK * (i + 1), js] = nt(eye, wt[js, BLK * i:BLK * (i + 1)]).astype(BF16)
    with scope("rs_chip3"):
        rs_chip_a(3)
        rs_chip_b(3)
    for t in range(steps + 1):
        with scope(f"DU_{t}"):
            if t < steps:
                du_tile(t)
            if t > 0:
                dx_tile(t - 1)
                dx_copy(t - 1).start()
        if t == 2:
            with scope("relay2"):
                rs_relay(2)

    def dg_copy(d):
        return pltpu.make_async_remote_copy(
            src_ref=dgslots.at[0], dst_ref=dgslots.at[d], send_sem=dg_send.at[d], recv_sem=dg_recv.at[d],
            device_id={"seq": lax.rem(me + d, n)}, device_id_type=MESH)

    dgrow = jnp.sum(jnp.transpose(dgacc[...]), axis=0, keepdims=True)
    dbrow = jnp.sum(jnp.transpose(dbacc[...]), axis=0, keepdims=True)
    dgslots[0] = jnp.concatenate([dgrow, dbrow], axis=0)
    for d in range(1, n):
        dg_copy(d).start()

    with scope("relay3"):
        rs_relay(3)
    with scope("final"):
        for u in range(3):
            rs_final(u)
    with scope("Y"):
        pl.loop(0, steps)(y_tile)
    with scope("final3"):
        rs_final(3)

    for d in range(1, n):
        dg_copy(d).wait_recv()
    total = dgslots[lax.rem(me, n)]
    for p in range(1, n):
        total = total + dgslots[lax.rem(me - p + n, n)]
    dg_ref[...] = total[0]
    db_ref[...] = total[1]

    for d in range(1, n):
        for e in range(4):
            ar1(e, d).wait_send()
            ar2(e, d).wait_send()
        dg_copy(d).wait_send()
    for u in range(4):
        out_copy(u).wait()
        for c in range(chips):
            d2d_copy(u, c).wait_send()
        for s in range(6):
            hop(u, s).wait_send()

    @pl.loop(0, steps)
    def _(t):
        y_copy(t).wait()
        dx_copy(t).wait()


def local_block(n, x_tok, dy_tok, ln_gamma, ln_beta, w_qkv, w_out):
    tokens, width = x_tok.shape
    _, three, heads, hd = w_qkv.shape
    wt = w_qkv.transpose(1, 2, 3, 0).reshape(three * width, width)
    steps = tokens // TT
    chips = n // 2
    own = width // n
    hbm = pl.BlockSpec(memory_space=pl.ANY)
    vmem = pl.BlockSpec(memory_space=pltpu.VMEM)
    gr = heads * hd // 4
    dma = pltpu.SemaphoreType.DMA
    y, dx, dwqkv, dwo, dg, db = pl.pallas_call(
        functools.partial(kernel, n, heads, hd),
        name="block",
        out_shape=(
            jax.ShapeDtypeStruct((tokens, width), BF16), jax.ShapeDtypeStruct((tokens, width), BF16),
            jax.ShapeDtypeStruct((own, three * width), F32), jax.ShapeDtypeStruct((own, width), F32),
            jax.ShapeDtypeStruct((width,), F32), jax.ShapeDtypeStruct((width,), F32)),
        in_specs=[hbm, hbm, vmem, vmem, hbm, hbm],
        out_specs=(hbm, hbm, hbm, hbm, vmem, vmem),
        scratch_shapes=[
            pltpu.VMEM((tokens, width), BF16), pltpu.VMEM((tokens, width), BF16),
            pltpu.VMEM((three * width, width), BF16), pltpu.VMEM((width, width), BF16),
            pltpu.VMEM((width, three * width), BF16),
            pltpu.VMEM((width, tokens), BF16), pltpu.VMEM((width, tokens), BF16), pltpu.VMEM((width, tokens), BF16),
            pltpu.VMEM((three * width, tokens), BF16), pltpu.VMEM((width, tokens), BF16),
            pltpu.VMEM((1, tokens), F32), pltpu.VMEM((1, tokens), F32),
            pltpu.VMEM((width, 128), F32), pltpu.VMEM((width, 128), F32),
            pltpu.VMEM((4, gr, BLK), F32), pltpu.VMEM((4, n, hd // 2, 128), F32),
            pltpu.VMEM((4, n, hd // 2, 128), F32), pltpu.VMEM((4, n, hd // 2, 128), F32),
            pltpu.VMEM((BLK, BLK), F32), pltpu.VMEM((4, gr, gr + 16), BF16), pltpu.VMEM((4, gr + 16, gr), BF16),
            pltpu.VMEM((2, width, TT), BF16),
            pltpu.VMEM((4, chips, 2, own, width), F32), pltpu.VMEM((4, chips, own, width), F32),
            pltpu.VMEM((4, 2, own // 2, width), F32), pltpu.VMEM((4, 2, own, width), F32),
            pltpu.VMEM((width, 128), F32), pltpu.VMEM((width, 128), F32), pltpu.VMEM((n, 2, width), F32),
            dma((3, max(steps, 3))), dma((3, max(steps, 4))),
            dma((8, n)), dma((8, n)), dma((4, chips + 6)), dma((4, chips + 6)), dma((n,)), dma((n,)),
        ],
        compiler_params=pltpu.CompilerParams(collective_id=0, has_side_effects=True, vmem_limit_bytes=67_000_000),
    )(x_tok, dy_tok, ln_gamma, ln_beta, wt, w_out)
    return y, dx, dwqkv.reshape(own, three, heads, hd), dwo, dg, db


def solution(mesh):
    rows = P(("data", "seq"), None)
    return jax.shard_map(
        functools.partial(local_block, mesh.shape["seq"]), mesh=mesh,
        in_specs=(rows, rows, P(None), P(None), P(None, None, None, None), P(None, None)),
        out_specs=(rows, rows, P(("data", "seq"), None, None, None), rows, P("data"), P("data")),
        check_vma=False)
```

```python
import functools

import jax
import jax.numpy as jnp
from jax import lax
from jax.experimental import pallas as pl
from jax.experimental.pallas import tpu as pltpu
from jax.sharding import PartitionSpec as P

LN_EPS = 1e-5
MESH = pl.DeviceIdType.MESH
F32 = jnp.float32
BF16 = jnp.bfloat16
TT = 512
BLK = 256


def nn(a, b):
    return lax.dot_general(a, b, (((1,), (0,)), ((), ())), preferred_element_type=F32)


def nt(a, b):
    return lax.dot_general(a, b, (((1,), (1,)), ((), ())), preferred_element_type=F32)


def kernel(n, heads, hd,
           x_hbm, dy_hbm, gam_ref, bet_ref, wt_hbm, wo_hbm,
           y_hbm, dx_hbm, dwqkv_hbm, dwo_hbm, dg_hbm, db_hbm,
           xbuf, dybuf, wt, wo, xT, dyT, uT, qkvT, oT, mean_ref, rstd_ref, gb, bb,
           s_acc, comp, ar_in, ar_out, sx, sg, sgt, ubuf,
           acc, d2d, relay, fin, dgacc, dgslots, dgout, dbout,
           sem_in, sem_out, ar_send, ar_recv, rs_send, rs_recv, dg_send, dg_recv):
    tokens, width = xbuf.shape
    steps = tokens // TT
    groups = 4
    hpg = heads // groups
    gr = hpg * hd
    nb = width // BLK
    chips = n // 2
    me = lax.axis_index("seq")
    chip, core = lax.div(me, 2), lax.rem(me, 2)
    partner = 2 * chip + (1 - core)
    c_right, c_left = lax.rem(chip + 1, chips), lax.rem(chip + chips - 1, chips)
    c_opp = lax.rem(chip + 2, chips)
    right, left = 2 * c_right + core, 2 * c_left + core

    def x_copy(t):
        r = pl.ds(pl.multiple_of(t * TT, TT), TT)
        return pltpu.make_async_copy(x_hbm.at[r, :], xbuf.at[r, :], sem_in.at[0, t])

    def dy_copy(t):
        r = pl.ds(pl.multiple_of(t * TT, TT), TT)
        return pltpu.make_async_copy(dy_hbm.at[r, :], dybuf.at[r, :], sem_in.at[1, t])

    wkv_copy = pltpu.make_async_copy(wt_hbm.at[pl.ds(width, 2 * width), :], wt.at[pl.ds(width, 2 * width), :], sem_in.at[2, 0])
    wq_copy = pltpu.make_async_copy(wt_hbm.at[pl.ds(0, width), :], wt.at[pl.ds(0, width), :], sem_in.at[2, 1])
    wo_copy = pltpu.make_async_copy(wo_hbm, wo, sem_in.at[2, 2])
    x_copy(0).start()
    wkv_copy.start()
    for t in range(1, steps):
        x_copy(t).start()
    for t in range(steps):
        dy_copy(t).start()
    wq_copy.start()
    wo_copy.start()

    barrier = pltpu.get_barrier_semaphore()
    for d in range(1, n):
        pl.semaphore_signal(barrier, inc=1, device_id={"seq": lax.rem(me + d, n)}, device_id_type=MESH)

    eye = (lax.broadcasted_iota(jnp.int32, (BLK, BLK), 0) == lax.broadcasted_iota(jnp.int32, (BLK, BLK), 1)).astype(F32).astype(BF16)
    gb[...] = jnp.transpose(jnp.broadcast_to(gam_ref[...][None, :], (128, width)))
    bb[...] = jnp.transpose(jnp.broadcast_to(bet_ref[...][None, :], (128, width)))
    s_acc[...] = jnp.zeros_like(s_acc)
    sx[...] = jnp.zeros_like(sx)
    dgacc[...] = jnp.zeros_like(dgacc)

    def lanes(ref_val, tt=TT):
        return jnp.concatenate([ref_val] * (tt // 128), axis=1)

    def fold(v):
        out = v[:, :128]
        for i in range(1, TT // 128):
            out = out + v[:, 128 * i:128 * (i + 1)]
        return out

    def tok(t, tt=TT):
        return pl.ds(t * tt if isinstance(t, int) else pl.multiple_of(t * tt, tt), tt)

    def phi(v32):
        ex = jnp.exp(jnp.minimum(v32, 0.0))
        pos = v32 > 0
        return jnp.where(pos, v32 + 1.0, ex).astype(BF16), jnp.where(pos, 1.0, ex)

    def parts3(v):
        p1 = v.astype(BF16).astype(F32)
        r = v - p1
        p2 = r.astype(BF16).astype(F32)
        return p1, p2, (r - p2).astype(BF16).astype(F32)

    scope = jax.named_scope
    ones_rows = jnp.ones((BLK - gr, TT), BF16)

    def norm_tile(t):
        ts = tok(t)
        xt = jnp.concatenate([nt(eye, xbuf[ts, BLK * b:BLK * (b + 1)]) for b in range(nb)], axis=0)
        xT[:, ts] = xt.astype(BF16)
        mean = jnp.sum(xt, axis=0, keepdims=True) * (1.0 / width)
        cen = xt - mean
        var = jnp.sum(cen * cen, axis=0, keepdims=True) * (1.0 / width)
        rstd = lax.rsqrt(var + LN_EPS)
        mean_ref[:, ts] = mean
        rstd_ref[:, ts] = rstd
        u = (cen * rstd * lanes(gb[...]) + lanes(bb[...])).astype(BF16)
        uT[:, ts] = u
        ubuf[t % 2] = u

    def kv_mm(t, half, u):
        ts = tok(t)
        hw = width // 2
        kb = nn(wt[width + hw * half:width + hw * (half + 1), :], u[...]).astype(BF16)
        vb = nn(wt[2 * width + hw * half:2 * width + hw * (half + 1), :], u[...]).astype(BF16)
        qkvT[width + hw * half:width + hw * (half + 1), ts] = kb
        qkvT[2 * width + hw * half:2 * width + hw * (half + 1), ts] = vb
        return half, phi(kb.astype(F32))[0], vb

    def s_mm(half, fk, vb):
        for i, g in enumerate(half_groups(half)):
            rows = slice(gr * i, gr * (i + 1))
            s_acc[g % 2] += nt(fk[rows], jnp.concatenate([vb[rows], ones_rows], axis=0))

    def half_groups(half):
        return range(groups // 2 * half, groups // 2 * (half + 1))

    lane128 = lax.broadcasted_iota(jnp.int32, (hd, 128), 1)
    lane256 = lax.broadcasted_iota(jnp.int32, (hd, BLK), 1)
    lane_sx = lax.broadcasted_iota(jnp.int32, (BLK, BLK), 1)
    rows_owned = hd // 2

    def compact(e, z_of):
        g0 = groups // 2 * (e % 2)

        def head(g, hh):
            blk = s_acc[g % 2, hd * hh:hd * (hh + 1), :]
            moved = pltpu.roll(blk, BLK - hd * hh, axis=1) if hh else blk
            return jnp.where(lane128 < hd, moved[:, :128], jnp.where(lane128 == hd, z_of(hh, blk), 0.0))

        if e >= 2:
            for d in range(1, n):
                ar1(e - 2, d).wait_send()
        for j in range(hpg):
            pair = head(g0, j) + pltpu.roll(head(g0 + 1, j), 64, axis=1)
            comp[e % 2, 2 * j] = pair[:rows_owned]
            comp[e % 2, 2 * j + 1] = pair[rows_owned:]
        s_acc[...] = jnp.zeros_like(s_acc)
        for d in range(1, n):
            ar1(e, d).start()

    def ar1(e, d):
        peer = lax.rem(me + d, n)
        return pltpu.make_async_remote_copy(
            src_ref=comp.at[e % 2, peer], dst_ref=ar_in.at[e % 2, d], send_sem=ar_send.at[2 * e, d], recv_sem=ar_recv.at[2 * e, d],
            device_id={"seq": peer}, device_id_type=MESH)

    def ar2(e, d):
        peer = lax.rem(me + d, n)
        return pltpu.make_async_remote_copy(
            src_ref=ar_out.at[e % 2, 0], dst_ref=ar_out.at[e % 2, d], send_sem=ar_send.at[2 * e + 1, d], recv_sem=ar_recv.at[2 * e + 1, d],
            device_id={"seq": peer}, device_id_type=MESH)

    def ar_reduce(e):
        total = comp[e % 2, me]
        for d in range(1, n):
            ar1(e, d).wait_recv()
            total = total + ar_in[e % 2, d]
            if e >= 2:
                ar2(e - 2, d).wait_send()
        ar_out[e % 2, 0] = total
        for d in range(1, n):
            ar2(e, d).start()

    def ar_finish(i):
        forward = i < 2
        for d in range(1, n):
            ar2(i, d).wait_recv()
        for g in half_groups(i % 2):
            for hh in range(hpg):
                part = jnp.concatenate([ar_out[i % 2, lax.rem(me - p + n, n)] for p in (2 * hh, 2 * hh + 1)], axis=0)
                if g % 2:
                    part = pltpu.roll(part, 64, axis=1)
                wide = jnp.concatenate([jnp.where(lane128 < hd, part, 0.0), jnp.zeros((hd, 128), F32)], axis=1)
                if hh:
                    wide = pltpu.roll(wide, hd * hh, axis=1)
                zc = part[:, hd:hd + 1]
                if forward:
                    hit = (lane256 == gr + hh) | (lane256 == gr + hpg + hh) | (lane256 == gr + 2 * hpg + hh)
                    wide = jnp.where(hit, jnp.broadcast_to(zc, (hd, BLK)), wide)
                else:
                    for j, zp in enumerate(parts3(jnp.broadcast_to(zc, (hd, BLK)))):
                        wide = jnp.where(lane256 == gr + j, zp, wide)
                sx[hd * hh:hd * (hh + 1), :] = wide
            m = sx[...]
            ext = jnp.where(lane_sx >= gr, -m, m) if forward else m
            sg[g] = ext[:gr, :gr + 16].astype(BF16)
            sgt[g] = jnp.transpose(m)[:gr + 16, :gr].astype(BF16)

    def z_fwd(hh, blk):
        return blk[:, gr:gr + 1]

    off = lane128 - (gr - 128)

    def z_bwd(hh, blk):
        hit = (off >= 0) & (off < 3 * hpg) & (lax.rem(off, hpg) == hh)
        return -jnp.sum(jnp.where(hit, blk[:, 128:], 0.0), axis=1, keepdims=True)

    def do_tile(t):
        acc[t, pl.ds(0, 2), :, :, :TT] = nn(wo[:width // 2, :], dyT[:, tok(t)]).reshape(2, 2, gr // 2, TT)

    def q_tile(t):
        ts = tok(t)
        dy_copy(t).wait()
        for b in range(nb):
            dyT[BLK * b:BLK * (b + 1), ts] = nt(eye, dybuf[ts, BLK * b:BLK * (b + 1)]).astype(BF16)
        qkvT[0:width, ts] = nn(wt[0:width, :], uT[:, ts]).astype(BF16)

    with scope("A0"):
        x_copy(0).wait()
        norm_tile(0)
    wkv_copy.wait()
    for t in range(steps):
        with scope(f"A_{t}"):
            if t + 1 < steps:
                x_copy(t + 1).wait()
                norm_tile(t + 1)
            now = kv_mm(t, 0, ubuf.at[t % 2])
            if t:
                s_mm(*last)
            last = now
    with scope("A_s"):
        s_mm(*last)
    pl.semaphore_wait(barrier, n - 1)
    with scope("compact0"):
        compact(0, z_fwd)
    with scope("A2"):
        @pl.loop(0, steps)
        def _(t):
            s_mm(*kv_mm(t, 1, uT.at[:, tok(t)]))
    with scope("compact1"):
        compact(1, z_fwd)

    wq_copy.wait()
    with scope("fill_q0"):
        q_tile(0)
    with scope("ar_reduce0"):
        ar_reduce(0)
    with scope("fill_q1"):
        pl.loop(1, steps)(q_tile)
    wo_copy.wait()
    with scope("do0"):
        pl.loop(0, steps)(do_tile)
    with scope("ar_reduce1"):
        ar_reduce(1)
    with scope("ar_finish0"):
        ar_finish(0)

    def per_head(v):
        return jnp.broadcast_to(v[:, None, :], (hpg, hd, TT)).reshape(gr, TT)

    def o_tiles(i, half):
        nds = [nn(sgt[g], phi(qkvT[gr * g:gr * (g + 1), tok(i)].astype(F32))[0]) for g in half_groups(half)]
        for g, nd in zip(half_groups(half), nds):
            oT[gr * g:gr * (g + 1), tok(i)] = (nd[:gr] * per_head(1.0 / nd[gr:gr + hpg])).astype(BF16)

    def b_tiles(i, half):
        pairs = [(i, g) for g in half_groups(half)]
        rows = {g: slice(gr * g, gr * (g + 1)) for _, g in pairs}
        feats = [phi(qkvT[rows[g], tok(t)].astype(F32)) for t, g in pairs]
        nds = [nn(sgt[g], fq) for (t, g), (fq, _) in zip(pairs, feats)]
        dos = [acc[t, g, :, :, :TT].reshape(gr, TT) if half == 0 else nn(wo[rows[g], :], dyT[:, tok(t)]) for t, g in pairs]
        ges = []
        for (t, g), nd, do in zip(pairs, nds, dos):
            rden = per_head(1.0 / nd[gr:gr + hpg])
            a = nd[:gr] * rden
            if half == 0:
                oT[rows[g], tok(t)] = a.astype(BF16)
            gg = (do * rden).astype(BF16)
            c = jnp.sum((gg.astype(F32) * a).reshape(hpg, hd, TT), axis=1)
            cp = jnp.concatenate(list(parts3(c)) + [jnp.zeros((hpg, TT), F32)], axis=0).astype(BF16)
            ges.append(jnp.concatenate([gg, cp], axis=0))
        dfqs = [nn(sg[g], ge) for (t, g), ge in zip(pairs, ges)]
        for (t, g), (fq, slope), ge, dfq in zip(pairs, feats, ges, dfqs):
            s_acc[g % 2] += nt(fq, jnp.concatenate([ge, jnp.zeros((BLK - gr - 16, TT), BF16)], axis=0))
            qkvT[rows[g], tok(t)] = (dfq * slope).astype(BF16)

    own = width // n

    def grad(u, between=None):
        @pl.loop(0, 2)
        def _(m):
            if between is not None:
                pl.when(m == 1)(between)
            half = lax.rem(lax.div(chip, 2) + 1 + m, 2)
            rs = pl.ds(pl.multiple_of(half * (width // 2), width // 2), width // 2)
            if u == 0:
                out = nn(oT[rs, :], dybuf[...])
            else:
                out = nt(uT[rs, :], qkvT[width * (u - 1):width * u, :])
            acc[u, pl.ds(2 * half, 2)] = out.reshape(2, 2, own, width)
            d2d_copy(u, 2 * half).start()
            d2d_copy(u, 2 * half + 1).start()

    hr = width // n // 2
    lo, hi = pl.ds(0, hr), pl.ds(hr, hr)

    def rdma(u, s, src, dst, peer):
        return pltpu.make_async_remote_copy(src_ref=src, dst_ref=dst, send_sem=rs_send.at[u, s], recv_sem=rs_recv.at[u, s],
                                            device_id={"seq": peer}, device_id_type=MESH)

    def d2d_copy(u, c):
        return rdma(u, c, acc.at[u, c, 1 - core], d2d.at[u, c], partner)

    def hop(u, s):
        if s == 0:
            return rdma(u, chips, acc.at[u, c_opp, core, lo], relay.at[u, 0], right)
        if s == 1:
            return rdma(u, chips + 1, acc.at[u, c_opp, core, hi], relay.at[u, 1], left)
        if s == 2:
            return rdma(u, chips + 2, acc.at[u, c_right, core, hi], fin.at[u, 0, hi], right)
        if s == 3:
            return rdma(u, chips + 3, acc.at[u, c_left, core, lo], fin.at[u, 1, lo], left)
        if s == 4:
            return rdma(u, chips + 4, acc.at[u, c_right, core, lo], fin.at[u, 0, lo], right)
        return rdma(u, chips + 5, acc.at[u, c_left, core, hi], fin.at[u, 1, hi], left)

    def rs_chip_a(u):
        d2d_copy(u, c_opp).wait_recv()
        acc[u, c_opp, core] += d2d[u, c_opp]
        hop(u, 0).start()
        hop(u, 1).start()

    def rs_chip_b(u):
        d2d_copy(u, c_right).wait_recv()
        acc[u, c_right, core] += d2d[u, c_right]
        hop(u, 2).start()
        d2d_copy(u, c_left).wait_recv()
        acc[u, c_left, core] += d2d[u, c_left]
        hop(u, 3).start()
        d2d_copy(u, chip).wait_recv()
        acc[u, chip, core] += d2d[u, chip]

    def rs_relay(u):
        hop(u, 0).wait_recv()
        acc[u, c_right, core, lo] += relay[u, 0]
        hop(u, 4).start()
        hop(u, 1).wait_recv()
        acc[u, c_left, core, hi] += relay[u, 1]
        hop(u, 5).start()

    def out_copy(u):
        if u == 0:
            return pltpu.make_async_copy(acc.at[u, chip, core], dwo_hbm, sem_out.at[2, u])
        return pltpu.make_async_copy((gb, dgacc, bb)[u - 1], dwqkv_hbm.at[pl.ds(width * (u - 1), width), :], sem_out.at[2, u])

    def rs_final(u):
        for s in range(2, 6):
            hop(u, s).wait_recv()
        total = acc[u, chip, core] + fin[u, 0] + fin[u, 1]
        if u == 0:
            acc[u, chip, core] = total
        else:
            (gb, dgacc, bb)[u - 1][:, :own] = jnp.transpose(total)
        out_copy(u).start()

    def y_copy(t):
        r = tok(t)
        return pltpu.make_async_copy(xbuf.at[r, :], y_hbm.at[r, :], sem_out.at[0, t])

    def dx_copy(t):
        r = tok(t)
        return pltpu.make_async_copy(dybuf.at[r, :], dx_hbm.at[r, :], sem_out.at[1, t])

    def store_tokens(buf, t, val):
        for s in range(TT // BLK):
            r = pl.ds(t * TT + BLK * s if isinstance(t, int) else pl.multiple_of(t * TT + BLK * s, BLK), BLK)
            for b in range(nb):
                buf[r, BLK * b:BLK * (b + 1)] = nt(eye, val[BLK * b:BLK * (b + 1), BLK * s:BLK * (s + 1)]).astype(BF16)

    def y_tile(t):
        ts = tok(t)
        yt = (nn(ubuf[0], oT[:TT, ts]) + nn(ubuf[1, :, :width - TT], oT[TT:, ts]) + xT[:, ts].astype(F32)).astype(BF16)
        store_tokens(xbuf, t, yt)
        y_copy(t).start()

    def c_tiles(i, half):
        pairs = [(2 * i + k, g) for k in range(2) for g in half_groups(half)]
        krows = {g: slice(width + gr * g, width + gr * (g + 1)) for _, g in pairs}
        vrows = {g: slice(2 * width + gr * g, 2 * width + gr * (g + 1)) for _, g in pairs}
        dfks = [nn(sg[g], jnp.concatenate([qkvT[vrows[g], tok(t)], ones_rows[:16]], axis=0)) for t, g in pairs]
        feats = [phi(qkvT[krows[g], tok(t)].astype(F32)) for t, g in pairs]
        dvs = [nn(sgt[g, :gr, :], fk) for (t, g), (fk, _) in zip(pairs, feats)]
        for (t, g), (_, slope), dfk, dv in zip(pairs, feats, dfks, dvs):
            qkvT[krows[g], tok(t)] = (dfk * slope).astype(BF16)
            qkvT[vrows[g], tok(t)] = dv.astype(BF16)

    def du_tile(t):
        i = 2 * (t % 2)
        d2d[i:i + 2, :, :, :TT] = (nn(dyT[...], qkvT[:tokens, tok(t)]) + nn(ubuf[1, :, BLK:], qkvT[tokens:, tok(t)])).reshape(2, chips, own, TT)

    def dx_tile(t):
        ts = tok(t)
        i = 2 * (t % 2)
        du = d2d[i:i + 2, :, :, :TT].reshape(width, TT)
        rstd = rstd_ref[:, ts]
        xhat = (xT[:, ts].astype(F32) - mean_ref[:, ts]) * rstd
        p = du * xhat
        dgacc[...] += fold(p)
        bb[...] += fold(du)
        gl = lanes(gb[...])
        e = du * gl
        m1 = jnp.sum(e, axis=0, keepdims=True) * (1.0 / width)
        m2 = jnp.sum(p * gl, axis=0, keepdims=True) * (1.0 / width)
        dyt = jnp.concatenate([nt(eye, dybuf[ts, BLK * b:BLK * (b + 1)]) for b in range(nb)], axis=0)
        dxt = (dyt + rstd * (e - m1 - xhat * m2)).astype(BF16)
        store_tokens(dybuf, t, dxt)

    def w_block(j):
        js = pl.ds(pl.multiple_of(j * BLK, BLK), BLK)
        for i in range(nb):
            dyT[BLK * i:BLK * (i + 1), js] = nt(eye, wt[js, BLK * i:BLK * (i + 1)]).astype(BF16)

    def w_rest():
        for i in range(nb):
            ubuf[1, BLK * i:BLK * (i + 1), BLK:] = nt(eye, wt[tokens:, BLK * i:BLK * (i + 1)]).astype(BF16)

    with scope("B0"):
        pl.loop(0, steps)(functools.partial(b_tiles, half=0))
    with scope("compact2"):
        compact(2, z_bwd)
    with scope("ar_finish1"):
        ar_finish(1)
    with scope("O1"):
        pl.loop(0, steps)(functools.partial(o_tiles, half=1))
    with scope("gradwo"):
        grad(0)
    with scope("ar_reduce2"):
        ar_reduce(2)
    with scope("rs_chip_a0"):
        rs_chip_a(0)
    with scope("B1"):
        @pl.loop(0, steps)
        def _(t):
            @pl.when(t == steps // 2)
            def _():
                rs_chip_b(0)
            b_tiles(t, half=1)
    with scope("compact3"):
        compact(3, z_bwd)
    with scope("fill_w"):
        pl.loop(0, tokens // BLK)(w_block)
        w_rest()
    with scope("relay0"):
        rs_relay(0)
    with scope("gradwq"):
        grad(1)
    with scope("ar_reduce3"):
        ar_reduce(3)
    with scope("chip_a1"):
        rs_chip_a(1)
    with scope("ar_finish2"):
        ar_finish(2)
    with scope("C0"):
        pl.loop(0, steps // 2)(functools.partial(c_tiles, half=0))
    with scope("rs_chip_b1"):
        rs_chip_b(1)
    with scope("fill_wo"):
        for i in range(nb):
            for j in range(nb):
                k = BLK * i // TT
                ubuf[k, BLK * j:BLK * (j + 1), BLK * i - TT * k:BLK * (i + 1) - TT * k] = nt(
                    eye, wo[BLK * i:BLK * (i + 1), BLK * j:BLK * (j + 1)]).astype(BF16)
    with scope("Y0"):
        pl.loop(0, steps // 2)(y_tile)
    with scope("ar_finish3"):
        ar_finish(3)
    with scope("C1"):
        pl.loop(0, steps // 2)(functools.partial(c_tiles, half=1))
    with scope("relay1"):
        rs_relay(1)
    with scope("gradwk"):
        grad(2)
    with scope("rs_chip_a2"):
        rs_chip_a(2)
    with scope("gradwv"):
        grad(3, lambda: rs_chip_b(2))
    with scope("rs_chip_a3"):
        rs_chip_a(3)
    bb[...] = jnp.zeros_like(bb)
    for t in range(steps + 1):
        with scope(f"DU_{t}"):
            if t < steps:
                du_tile(t)
            if t > 0:
                dx_tile(t - 1)
                dx_copy(t - 1).start()
        if t == 0:
            with scope("relay2"):
                rs_chip_b(3)
                rs_relay(2)
        if t == 2:
            with scope("relay3"):
                rs_relay(3)

    def dg_copy(d):
        return pltpu.make_async_remote_copy(
            src_ref=dgslots.at[0], dst_ref=dgslots.at[d], send_sem=dg_send.at[d], recv_sem=dg_recv.at[d],
            device_id={"seq": lax.rem(me + d, n)}, device_id_type=MESH)

    dgrow = jnp.sum(jnp.transpose(dgacc[...]), axis=0, keepdims=True)
    dbrow = jnp.sum(jnp.transpose(bb[...]), axis=0, keepdims=True)
    dgslots[0] = jnp.concatenate([dgrow, dbrow], axis=0)
    for d in range(1, n):
        dg_copy(d).start()

    def dg_out(i):
        return pltpu.make_async_copy((dgout, dbout)[i], (dg_hbm, db_hbm)[i], sem_out.at[3, i])

    with scope("final"):
        rs_final(0)
        rs_final(1)
    with scope("Y1"):
        pl.loop(steps // 2, steps)(y_tile)
    with scope("final2"):
        rs_final(2)
    with scope("final3"):
        rs_final(3)

    with scope("dg"):
        for d in range(1, n):
            dg_copy(d).wait_recv()
        total = dgslots[me]
        for p in range(1, n):
            total = total + dgslots[lax.rem(me - p + n, n)]
        dgout[...] = total[0]
        dbout[...] = total[1]
        dg_out(0).start()
        dg_out(1).start()
    dg_out(0).wait()
    dg_out(1).wait()
    for d in range(1, n):
        for e in (2, 3):
            ar1(e, d).wait_send()
            ar2(e, d).wait_send()
        dg_copy(d).wait_send()
    for u in range(4):
        out_copy(u).wait()
        for c in range(chips):
            d2d_copy(u, c).wait_send()
        for s in range(6):
            hop(u, s).wait_send()

    @pl.loop(0, steps)
    def _(t):
        y_copy(t).wait()
        dx_copy(t).wait()


def local_block(n, x_tok, dy_tok, ln_gamma, ln_beta, w_qkv, w_out):
    tokens, width = x_tok.shape
    _, three, heads, hd = w_qkv.shape
    wt = w_qkv.transpose(1, 2, 3, 0).reshape(three * width, width)
    steps = tokens // TT
    chips = n // 2
    own = width // n
    hbm = pl.BlockSpec(memory_space=pl.ANY)
    vmem = pl.BlockSpec(memory_space=pltpu.VMEM)
    gr = heads * hd // 4
    dma = pltpu.SemaphoreType.DMA
    y, dx, dwqkv, dwo, dg, db = pl.pallas_call(
        functools.partial(kernel, n, heads, hd),
        name="block",
        out_shape=(
            jax.ShapeDtypeStruct((tokens, width), BF16), jax.ShapeDtypeStruct((tokens, width), BF16),
            jax.ShapeDtypeStruct((three * width, 128), F32), jax.ShapeDtypeStruct((own, width), F32),
            jax.ShapeDtypeStruct((width,), F32), jax.ShapeDtypeStruct((width,), F32)),
        in_specs=[hbm, hbm, vmem, vmem, hbm, hbm],
        out_specs=(hbm,) * 6,
        scratch_shapes=[
            pltpu.VMEM((tokens, width), BF16), pltpu.VMEM((tokens, width), BF16),
            pltpu.VMEM((three * width, width), BF16), pltpu.VMEM((width, width), BF16),
            pltpu.VMEM((width, tokens), BF16), pltpu.VMEM((width, tokens), BF16), pltpu.VMEM((width, tokens), BF16),
            pltpu.VMEM((three * width, tokens), BF16), pltpu.VMEM((width, tokens), BF16),
            pltpu.VMEM((1, tokens), F32), pltpu.VMEM((1, tokens), F32),
            pltpu.VMEM((width, 128), F32), pltpu.VMEM((width, 128), F32),
            pltpu.VMEM((2, gr, BLK), F32), pltpu.VMEM((2, n, hd // 2, 128), F32),
            pltpu.VMEM((2, n, hd // 2, 128), F32), pltpu.VMEM((2, n, hd // 2, 128), F32),
            pltpu.VMEM((BLK, BLK), F32), pltpu.VMEM((4, gr, gr + 16), BF16), pltpu.VMEM((4, gr + 16, gr), BF16),
            pltpu.VMEM((2, width, TT), BF16),
            pltpu.VMEM((4, chips, 2, own, width), F32), pltpu.VMEM((4, chips, own, width), F32),
            pltpu.VMEM((4, 2, own // 2, width), F32), pltpu.VMEM((4, 2, own, width), F32),
            pltpu.VMEM((width, 128), F32), pltpu.VMEM((n, 2, width), F32), pltpu.VMEM((width,), F32), pltpu.VMEM((width,), F32),
            dma((3, max(steps, 3))), dma((4, max(steps, 4))),
            dma((8, n)), dma((8, n)), dma((4, chips + 6)), dma((4, chips + 6)), dma((n,)), dma((n,)),
        ],
        compiler_params=pltpu.CompilerParams(collective_id=0, has_side_effects=True, vmem_limit_bytes=67_000_000),
    )(x_tok, dy_tok, ln_gamma, ln_beta, wt, w_out)
    return y, dx, dwqkv[:, :own].reshape(three, heads, hd, own).transpose(3, 0, 1, 2), dwo, dg, db


def solution(mesh):
    rows = P(("data", "seq"), None)
    return jax.shard_map(
        functools.partial(local_block, mesh.shape["seq"]), mesh=mesh,
        in_specs=(rows, rows, P(None), P(None), P(None, None, None, None), P(None, None)),
        out_specs=(rows, rows, P(("data", "seq"), None, None, None), rows, P("data"), P("data")),
        check_vma=False)
```

```python
import functools

import jax
import jax.numpy as jnp
from jax import lax
from jax.experimental import pallas as pl
from jax.experimental.pallas import tpu as pltpu
from jax.sharding import PartitionSpec as P

LN_EPS = 1e-5
MESH = pl.DeviceIdType.MESH
F32 = jnp.float32
BF16 = jnp.bfloat16
TT = 512
BLK = 256


def nn(a, b):
    return lax.dot_general(a, b, (((1,), (0,)), ((), ())), preferred_element_type=F32)


def nt(a, b):
    return lax.dot_general(a, b, (((1,), (1,)), ((), ())), preferred_element_type=F32)


def kernel(n, heads, hd,
           x_hbm, dy_hbm, gam_ref, bet_ref, wt_hbm, wo_hbm,
           y_hbm, dx_hbm, dwqkv_hbm, dwo_hbm, dg_hbm, db_hbm,
           xbuf, dybuf, wt, wo, xT, dyT, uT, qkvT, oT, mean_ref, rstd_ref, gb, bb,
           s_acc, comp, ar_in, ar_out, sx, sg, sgt, ubuf,
           acc, d2d, relay, fin, dgacc, dgslots, dgout, dbout,
           sem_in, sem_out, ar_send, ar_recv, rs_send, rs_recv, dg_send, dg_recv):
    tokens, width = xbuf.shape
    steps = tokens // TT
    groups = 4
    hpg = heads // groups
    gr = hpg * hd
    nb = width // BLK
    chips = n // 2
    me = lax.axis_index("seq")
    chip, core = lax.div(me, 2), lax.rem(me, 2)
    partner = 2 * chip + (1 - core)
    c_right, c_left = lax.rem(chip + 1, chips), lax.rem(chip + chips - 1, chips)
    c_opp = lax.rem(chip + 2, chips)
    right, left = 2 * c_right + core, 2 * c_left + core

    def x_copy(t):
        r = pl.ds(pl.multiple_of(t * TT, TT), TT)
        return pltpu.make_async_copy(x_hbm.at[r, :], xbuf.at[r, :], sem_in.at[0, t])

    def dy_copy(t):
        r = pl.ds(pl.multiple_of(t * TT, TT), TT)
        return pltpu.make_async_copy(dy_hbm.at[r, :], dybuf.at[r, :], sem_in.at[1, t])

    wkv_copy = pltpu.make_async_copy(wt_hbm.at[pl.ds(width, 2 * width), :], wt.at[pl.ds(width, 2 * width), :], sem_in.at[2, 0])
    wq_copy = pltpu.make_async_copy(wt_hbm.at[pl.ds(0, width), :], wt.at[pl.ds(0, width), :], sem_in.at[2, 1])
    wo_copy = pltpu.make_async_copy(wo_hbm, wo, sem_in.at[2, 2])
    x_copy(0).start()
    wkv_copy.start()
    for t in range(1, steps):
        x_copy(t).start()
    for t in range(steps):
        dy_copy(t).start()
    wq_copy.start()
    wo_copy.start()

    barrier = pltpu.get_barrier_semaphore()
    for d in range(1, n):
        pl.semaphore_signal(barrier, inc=1, device_id={"seq": lax.rem(me + d, n)}, device_id_type=MESH)

    eye = (lax.broadcasted_iota(jnp.int32, (BLK, BLK), 0) == lax.broadcasted_iota(jnp.int32, (BLK, BLK), 1)).astype(F32).astype(BF16)
    gb[...] = jnp.transpose(jnp.broadcast_to(gam_ref[...][None, :], (128, width)))
    bb[...] = jnp.transpose(jnp.broadcast_to(bet_ref[...][None, :], (128, width)))
    s_acc[...] = jnp.zeros_like(s_acc)
    sx[...] = jnp.zeros_like(sx)
    dgacc[...] = jnp.zeros_like(dgacc)

    def lanes(ref_val, tt=TT):
        return jnp.concatenate([ref_val] * (tt // 128), axis=1)

    def fold(v):
        out = v[:, :128]
        for i in range(1, TT // 128):
            out = out + v[:, 128 * i:128 * (i + 1)]
        return out

    def tok(t, tt=TT):
        return pl.ds(t * tt if isinstance(t, int) else pl.multiple_of(t * tt, tt), tt)

    def phi(v32):
        ex = jnp.exp(jnp.minimum(v32, 0.0))
        pos = v32 > 0
        return jnp.where(pos, v32 + 1.0, ex).astype(BF16), jnp.where(pos, 1.0, ex)

    def parts3(v):
        p1 = v.astype(BF16).astype(F32)
        r = v - p1
        p2 = r.astype(BF16).astype(F32)
        return p1, p2, (r - p2).astype(BF16).astype(F32)

    scope = jax.named_scope
    ones_rows = jnp.ones((BLK - gr, TT), BF16)

    def norm_tile(t):
        ts = tok(t)
        xt = jnp.concatenate([nt(eye, xbuf[ts, BLK * b:BLK * (b + 1)]) for b in range(nb)], axis=0)
        xT[:, ts] = xt.astype(BF16)
        mean = jnp.sum(xt, axis=0, keepdims=True) * (1.0 / width)
        cen = xt - mean
        var = jnp.sum(cen * cen, axis=0, keepdims=True) * (1.0 / width)
        rstd = lax.rsqrt(var + LN_EPS)
        mean_ref[:, ts] = mean
        rstd_ref[:, ts] = rstd
        u = (cen * rstd * lanes(gb[...]) + lanes(bb[...])).astype(BF16)
        uT[:, ts] = u
        ubuf[t % 2] = u

    def kv_mm(t, half, u):
        ts = tok(t)
        hw = width // 2
        kb = nn(wt[width + hw * half:width + hw * (half + 1), :], u[...]).astype(BF16)
        vb = nn(wt[2 * width + hw * half:2 * width + hw * (half + 1), :], u[...]).astype(BF16)
        qkvT[width + hw * half:width + hw * (half + 1), ts] = kb
        qkvT[2 * width + hw * half:2 * width + hw * (half + 1), ts] = vb
        return half, phi(kb.astype(F32))[0], vb

    def s_mm(half, fk, vb):
        for i, g in enumerate(half_groups(half)):
            rows = slice(gr * i, gr * (i + 1))
            s_acc[g % 2] += nt(fk[rows], jnp.concatenate([vb[rows], ones_rows], axis=0))

    def half_groups(half):
        return range(groups // 2 * half, groups // 2 * (half + 1))

    lane128 = lax.broadcasted_iota(jnp.int32, (hd, 128), 1)
    lane256 = lax.broadcasted_iota(jnp.int32, (hd, BLK), 1)
    lane_sx = lax.broadcasted_iota(jnp.int32, (BLK, BLK), 1)
    rows_owned = hd // 2

    def compact(e, z_of):
        g0 = groups // 2 * (e % 2)

        def head(g, hh):
            blk = s_acc[g % 2, hd * hh:hd * (hh + 1), :]
            moved = pltpu.roll(blk, BLK - hd * hh, axis=1) if hh else blk
            return jnp.where(lane128 < hd, moved[:, :128], jnp.where(lane128 == hd, z_of(hh, blk), 0.0))

        if e >= 2:
            for d in range(1, n):
                ar1(e - 2, d).wait_send()
        for j in range(hpg):
            pair = head(g0, j) + pltpu.roll(head(g0 + 1, j), 64, axis=1)
            comp[e % 2, 2 * j] = pair[:rows_owned]
            comp[e % 2, 2 * j + 1] = pair[rows_owned:]
        s_acc[...] = jnp.zeros_like(s_acc)
        for d in range(1, n):
            ar1(e, d).start()

    def ar1(e, d):
        peer = lax.rem(me + d, n)
        return pltpu.make_async_remote_copy(
            src_ref=comp.at[e % 2, peer], dst_ref=ar_in.at[e % 2, d], send_sem=ar_send.at[2 * (e % 2), d - 1], recv_sem=ar_recv.at[2 * (e % 2), d - 1],
            device_id={"seq": peer}, device_id_type=MESH)

    def ar2(e, d):
        peer = lax.rem(me + d, n)
        return pltpu.make_async_remote_copy(
            src_ref=ar_out.at[e % 2, 0], dst_ref=ar_out.at[e % 2, d], send_sem=ar_send.at[2 * (e % 2) + 1, d - 1], recv_sem=ar_recv.at[2 * (e % 2) + 1, d - 1],
            device_id={"seq": peer}, device_id_type=MESH)

    def ar_reduce(e):
        total = comp[e % 2, me]
        for d in range(1, n):
            ar1(e, d).wait_recv()
            total = total + ar_in[e % 2, d]
            if e >= 2:
                ar2(e - 2, d).wait_send()
        ar_out[e % 2, 0] = total
        for d in range(1, n):
            ar2(e, d).start()

    def ar_finish(i):
        forward = i < 2
        for d in range(1, n):
            ar2(i, d).wait_recv()
        for g in half_groups(i % 2):
            for hh in range(hpg):
                part = jnp.concatenate([ar_out[i % 2, lax.rem(me - p + n, n)] for p in (2 * hh, 2 * hh + 1)], axis=0)
                if g % 2:
                    part = pltpu.roll(part, 64, axis=1)
                wide = jnp.concatenate([jnp.where(lane128 < hd, part, 0.0), jnp.zeros((hd, 128), F32)], axis=1)
                if hh:
                    wide = pltpu.roll(wide, hd * hh, axis=1)
                zc = part[:, hd:hd + 1]
                if forward:
                    hit = (lane256 == gr + hh) | (lane256 == gr + hpg + hh) | (lane256 == gr + 2 * hpg + hh)
                    wide = jnp.where(hit, jnp.broadcast_to(zc, (hd, BLK)), wide)
                else:
                    for j, zp in enumerate(parts3(jnp.broadcast_to(zc, (hd, BLK)))):
                        wide = jnp.where(lane256 == gr + j, zp, wide)
                sx[hd * hh:hd * (hh + 1), :] = wide
            m = sx[...]
            ext = jnp.where(lane_sx >= gr, -m, m) if forward else m
            sg[g] = ext[:gr, :gr + 16].astype(BF16)
            sgt[g] = jnp.transpose(m)[:gr + 16, :gr].astype(BF16)

    def z_fwd(hh, blk):
        return blk[:, gr:gr + 1]

    off = lane128 - (gr - 128)

    def z_bwd(hh, blk):
        hit = (off >= 0) & (off < 3 * hpg) & (lax.rem(off, hpg) == hh)
        return -jnp.sum(jnp.where(hit, blk[:, 128:], 0.0), axis=1, keepdims=True)

    def do_tile(t):
        acc[t, pl.ds(0, 2), :, :, :TT] = nn(wo[:width // 2, :], dyT[:, tok(t)]).reshape(2, 2, gr // 2, TT)

    def q_tile(t):
        ts = tok(t)
        dy_copy(t).wait()
        for b in range(nb):
            dyT[BLK * b:BLK * (b + 1), ts] = nt(eye, dybuf[ts, BLK * b:BLK * (b + 1)]).astype(BF16)
        qkvT[0:width, ts] = nn(wt[0:width, :], uT[:, ts]).astype(BF16)

    with scope("A0"):
        x_copy(0).wait()
        norm_tile(0)
    wkv_copy.wait()
    for t in range(steps):
        with scope(f"A_{t}"):
            if t + 1 < steps:
                x_copy(t + 1).wait()
                norm_tile(t + 1)
            now = kv_mm(t, 0, ubuf.at[t % 2])
            if t:
                s_mm(*last)
            last = now
    with scope("A_s"):
        s_mm(*last)
    pl.semaphore_wait(barrier, n - 1)
    with scope("compact0"):
        compact(0, z_fwd)
    with scope("A2"):
        @pl.loop(0, steps)
        def _(t):
            s_mm(*kv_mm(t, 1, uT.at[:, tok(t)]))
    with scope("compact1"):
        compact(1, z_fwd)

    wq_copy.wait()
    with scope("fill_q0"):
        q_tile(0)
    with scope("ar_reduce0"):
        ar_reduce(0)
    with scope("fill_q1"):
        pl.loop(1, steps)(q_tile)
    wo_copy.wait()
    with scope("do0"):
        pl.loop(0, steps)(do_tile)
    with scope("ar_reduce1"):
        ar_reduce(1)
    with scope("ar_finish0"):
        ar_finish(0)

    def per_head(v):
        return jnp.broadcast_to(v[:, None, :], (hpg, hd, TT)).reshape(gr, TT)

    def o_tiles(i, half):
        nds = [nn(sgt[g], phi(qkvT[gr * g:gr * (g + 1), tok(i)].astype(F32))[0]) for g in half_groups(half)]
        for g, nd in zip(half_groups(half), nds):
            oT[gr * g:gr * (g + 1), tok(i)] = (nd[:gr] * per_head(1.0 / nd[gr:gr + hpg])).astype(BF16)

    def b_tiles(i, half):
        pairs = [(i, g) for g in half_groups(half)]
        rows = {g: slice(gr * g, gr * (g + 1)) for _, g in pairs}
        feats = [phi(qkvT[rows[g], tok(t)].astype(F32)) for t, g in pairs]
        nds = [nn(sgt[g], fq) for (t, g), (fq, _) in zip(pairs, feats)]
        dos = [acc[t, g, :, :, :TT].reshape(gr, TT) if half == 0 else nn(wo[rows[g], :], dyT[:, tok(t)]) for t, g in pairs]
        ges = []
        for (t, g), nd, do in zip(pairs, nds, dos):
            rden = per_head(1.0 / nd[gr:gr + hpg])
            a = nd[:gr] * rden
            if half == 0:
                oT[rows[g], tok(t)] = a.astype(BF16)
            gg = (do * rden).astype(BF16)
            c = jnp.sum((gg.astype(F32) * a).reshape(hpg, hd, TT), axis=1)
            cp = jnp.concatenate(list(parts3(c)) + [jnp.zeros((hpg, TT), F32)], axis=0).astype(BF16)
            ges.append(jnp.concatenate([gg, cp], axis=0))
        dfqs = [nn(sg[g], ge) for (t, g), ge in zip(pairs, ges)]
        for (t, g), (fq, slope), ge, dfq in zip(pairs, feats, ges, dfqs):
            s_acc[g % 2] += nt(fq, jnp.concatenate([ge, jnp.zeros((BLK - gr - 16, TT), BF16)], axis=0))
            qkvT[rows[g], tok(t)] = (dfq * slope).astype(BF16)

    own = width // n

    def grad(u, between=None):
        @pl.loop(0, 2)
        def _(m):
            if between is not None:
                pl.when(m == 1)(between)
            half = lax.rem(lax.div(chip, 2) + 1 + m, 2)
            rs = pl.ds(pl.multiple_of(half * (width // 2), width // 2), width // 2)
            if u == 0:
                out = nn(oT[rs, :], dybuf[...])
            else:
                out = nt(uT[rs, :], qkvT[width * (u - 1):width * u, :])
            acc[u, pl.ds(2 * half, 2)] = out.reshape(2, 2, own, width)
            d2d_copy(u, 2 * half).start()
            d2d_copy(u, 2 * half + 1).start()

    hr = width // n // 2
    lo, hi = pl.ds(0, hr), pl.ds(hr, hr)

    def rdma(u, s, src, dst, peer):
        return pltpu.make_async_remote_copy(src_ref=src, dst_ref=dst, send_sem=rs_send.at[u, s], recv_sem=rs_recv.at[u, s],
                                            device_id={"seq": peer}, device_id_type=MESH)

    def d2d_copy(u, c):
        return rdma(u, c, acc.at[u, c, 1 - core], d2d.at[u, c], partner)

    def hop(u, s):
        if s == 0:
            return rdma(u, chips, acc.at[u, c_opp, core, lo], relay.at[u, 0], right)
        if s == 1:
            return rdma(u, chips + 1, acc.at[u, c_opp, core, hi], relay.at[u, 1], left)
        if s == 2:
            return rdma(u, chips + 2, acc.at[u, c_right, core, hi], fin.at[u, 0, hi], right)
        if s == 3:
            return rdma(u, chips + 3, acc.at[u, c_left, core, lo], fin.at[u, 1, lo], left)
        if s == 4:
            return rdma(u, chips + 4, acc.at[u, c_right, core, lo], fin.at[u, 0, lo], right)
        return rdma(u, chips + 5, acc.at[u, c_left, core, hi], fin.at[u, 1, hi], left)

    def rs_chip_a(u):
        d2d_copy(u, c_opp).wait_recv()
        acc[u, c_opp, core] += d2d[u, c_opp]
        hop(u, 0).start()
        hop(u, 1).start()

    def rs_chip_b(u):
        d2d_copy(u, c_right).wait_recv()
        acc[u, c_right, core] += d2d[u, c_right]
        hop(u, 2).start()
        d2d_copy(u, c_left).wait_recv()
        acc[u, c_left, core] += d2d[u, c_left]
        hop(u, 3).start()
        d2d_copy(u, chip).wait_recv()
        acc[u, chip, core] += d2d[u, chip]

    def rs_relay(u):
        hop(u, 0).wait_recv()
        acc[u, c_right, core, lo] += relay[u, 0]
        hop(u, 4).start()
        hop(u, 1).wait_recv()
        acc[u, c_left, core, hi] += relay[u, 1]
        hop(u, 5).start()

    def out_copy(u):
        if u == 0:
            return pltpu.make_async_copy(acc.at[u, chip, core], dwo_hbm, sem_out.at[2, u])
        return pltpu.make_async_copy((gb, dgacc, bb)[u - 1], dwqkv_hbm.at[pl.ds(width * (u - 1), width), :], sem_out.at[2, u])

    def rs_final(u):
        for s in range(2, 6):
            hop(u, s).wait_recv()
        total = acc[u, chip, core] + fin[u, 0] + fin[u, 1]
        if u == 0:
            acc[u, chip, core] = total
        else:
            (gb, dgacc, bb)[u - 1][:, :own] = jnp.transpose(total)
        out_copy(u).start()

    def y_copy(t):
        r = tok(t)
        return pltpu.make_async_copy(xbuf.at[r, :], y_hbm.at[r, :], sem_out.at[0, t])

    def dx_copy(t):
        r = tok(t)
        return pltpu.make_async_copy(dybuf.at[r, :], dx_hbm.at[r, :], sem_out.at[1, t])

    def store_tokens(buf, t, val):
        for s in range(TT // BLK):
            r = pl.ds(t * TT + BLK * s if isinstance(t, int) else pl.multiple_of(t * TT + BLK * s, BLK), BLK)
            for b in range(nb):
                buf[r, BLK * b:BLK * (b + 1)] = nt(eye, val[BLK * b:BLK * (b + 1), BLK * s:BLK * (s + 1)]).astype(BF16)

    def y_tile(t):
        ts = tok(t)
        yt = (nn(ubuf[0], oT[:TT, ts]) + nn(ubuf[1, :, :width - TT], oT[TT:, ts]) + xT[:, ts].astype(F32)).astype(BF16)
        store_tokens(xbuf, t, yt)
        y_copy(t).start()

    def c_tiles(i, half):
        pairs = [(2 * i + k, g) for k in range(2) for g in half_groups(half)]
        krows = {g: slice(width + gr * g, width + gr * (g + 1)) for _, g in pairs}
        vrows = {g: slice(2 * width + gr * g, 2 * width + gr * (g + 1)) for _, g in pairs}
        dfks = [nn(sg[g], jnp.concatenate([qkvT[vrows[g], tok(t)], ones_rows[:16]], axis=0)) for t, g in pairs]
        feats = [phi(qkvT[krows[g], tok(t)].astype(F32)) for t, g in pairs]
        dvs = [nn(sgt[g, :gr, :], fk) for (t, g), (fk, _) in zip(pairs, feats)]
        for (t, g), (_, slope), dfk, dv in zip(pairs, feats, dfks, dvs):
            qkvT[krows[g], tok(t)] = (dfk * slope).astype(BF16)
            qkvT[vrows[g], tok(t)] = dv.astype(BF16)

    def du_tile(t):
        i = 2 * (t % 2)
        d2d[i:i + 2, :, :, :TT] = (nn(dyT[...], qkvT[:tokens, tok(t)]) + nn(ubuf[1, :, BLK:], qkvT[tokens:, tok(t)])).reshape(2, chips, own, TT)

    def dx_tile(t):
        ts = tok(t)
        i = 2 * (t % 2)
        du = d2d[i:i + 2, :, :, :TT].reshape(width, TT)
        rstd = rstd_ref[:, ts]
        xhat = (xT[:, ts].astype(F32) - mean_ref[:, ts]) * rstd
        p = du * xhat
        dgacc[...] += fold(p)
        bb[...] += fold(du)
        gl = lanes(gb[...])
        e = du * gl
        m1 = jnp.sum(e, axis=0, keepdims=True) * (1.0 / width)
        m2 = jnp.sum(p * gl, axis=0, keepdims=True) * (1.0 / width)
        dxt = (uT[:, ts].astype(F32) + rstd * (e - m1 - xhat * m2)).astype(BF16)
        store_tokens(dybuf, t, dxt)

    def w_block(j):
        js = pl.ds(pl.multiple_of(j * BLK, BLK), BLK)
        for i in range(nb):
            dyT[BLK * i:BLK * (i + 1), js] = nt(eye, wt[js, BLK * i:BLK * (i + 1)]).astype(BF16)

    def w_rest():
        for i in range(nb):
            ubuf[1, BLK * i:BLK * (i + 1), BLK:] = nt(eye, wt[tokens:, BLK * i:BLK * (i + 1)]).astype(BF16)

    with scope("B0"):
        pl.loop(0, steps)(functools.partial(b_tiles, half=0))
    with scope("compact2"):
        compact(2, z_bwd)
    with scope("ar_finish1"):
        ar_finish(1)
    with scope("O1"):
        pl.loop(0, steps)(functools.partial(o_tiles, half=1))
    with scope("gradwo"):
        grad(0)
    with scope("ar_reduce2"):
        ar_reduce(2)
    with scope("rs_chip_a0"):
        rs_chip_a(0)
    with scope("B1"):
        @pl.loop(0, steps)
        def _(t):
            @pl.when(t == steps // 2)
            def _():
                rs_chip_b(0)
            b_tiles(t, half=1)
    with scope("compact3"):
        compact(3, z_bwd)
    with scope("fill_w"):
        pl.loop(0, tokens // BLK)(w_block)
        w_rest()
    with scope("relay0"):
        rs_relay(0)
    with scope("gradwq"):
        grad(1)
    with scope("ar_reduce3"):
        ar_reduce(3)
    with scope("chip_a1"):
        rs_chip_a(1)
    with scope("ar_finish2"):
        ar_finish(2)
    with scope("C0"):
        pl.loop(0, steps // 2)(functools.partial(c_tiles, half=0))
    with scope("rs_chip_b1"):
        rs_chip_b(1)
    with scope("fill_wo"):
        for i in range(nb):
            for j in range(nb):
                k = BLK * i // TT
                ubuf[k, BLK * j:BLK * (j + 1), BLK * i - TT * k:BLK * (i + 1) - TT * k] = nt(
                    eye, wo[BLK * i:BLK * (i + 1), BLK * j:BLK * (j + 1)]).astype(BF16)
    with scope("Y0"):
        pl.loop(0, steps // 2)(y_tile)
    with scope("ar_finish3"):
        ar_finish(3)
    with scope("C1"):
        pl.loop(0, steps // 2)(functools.partial(c_tiles, half=1))
    with scope("relay1"):
        rs_relay(1)
    with scope("gradwk"):
        grad(2)
    with scope("rs_chip_a2"):
        rs_chip_a(2)
    with scope("gradwv"):
        grad(3, lambda: rs_chip_b(2))
    with scope("rs_chip_a3"):
        rs_chip_a(3)
    bb[...] = jnp.zeros_like(bb)
    for t in range(steps + 1):
        with scope(f"DU_{t}"):
            if t > 0:
                for b in range(nb):
                    uT[BLK * b:BLK * (b + 1), tok(t - 1)] = nt(eye, dybuf[tok(t - 1), BLK * b:BLK * (b + 1)]).astype(BF16)
            if t < steps:
                du_tile(t)
            if t > 0:
                dx_tile(t - 1)
                dx_copy(t - 1).start()
        if t == 0:
            with scope("relay2"):
                rs_chip_b(3)
                rs_relay(2)
        if t == 2:
            with scope("relay3"):
                rs_relay(3)

    def dg_copy(d):
        return pltpu.make_async_remote_copy(
            src_ref=dgslots.at[0], dst_ref=dgslots.at[d], send_sem=dg_send.at[d - 1], recv_sem=dg_recv.at[d - 1],
            device_id={"seq": lax.rem(me + d, n)}, device_id_type=MESH)

    dgrow = jnp.sum(jnp.transpose(dgacc[...]), axis=0, keepdims=True)
    dbrow = jnp.sum(jnp.transpose(bb[...]), axis=0, keepdims=True)
    dgslots[0] = jnp.concatenate([dgrow, dbrow], axis=0)
    for d in range(1, n):
        dg_copy(d).start()

    def dg_out(i):
        return pltpu.make_async_copy((dgout, dbout)[i], (dg_hbm, db_hbm)[i], sem_out.at[3, i])

    with scope("final"):
        rs_final(0)
        rs_final(1)
    with scope("Y1"):
        pl.loop(steps // 2, steps)(y_tile)
    with scope("final2"):
        rs_final(2)
    with scope("final3"):
        rs_final(3)

    with scope("dg"):
        for d in range(1, n):
            dg_copy(d).wait_recv()
        total = dgslots[me]
        for p in range(1, n):
            total = total + dgslots[lax.rem(me - p + n, n)]
        dgout[...] = total[0]
        dbout[...] = total[1]
        dg_out(0).start()
        dg_out(1).start()
    dg_out(0).wait()
    dg_out(1).wait()
    for d in range(1, n):
        for e in (2, 3):
            ar1(e, d).wait_send()
            ar2(e, d).wait_send()
        dg_copy(d).wait_send()
    for u in range(4):
        out_copy(u).wait()
        for c in range(chips):
            d2d_copy(u, c).wait_send()
        for s in range(6):
            hop(u, s).wait_send()

    @pl.loop(0, steps)
    def _(t):
        y_copy(t).wait()
        dx_copy(t).wait()


def local_block(n, x_tok, dy_tok, ln_gamma, ln_beta, w_qkv, w_out):
    tokens, width = x_tok.shape
    _, three, heads, hd = w_qkv.shape
    wt = w_qkv.transpose(1, 2, 3, 0).reshape(three * width, width)
    steps = tokens // TT
    chips = n // 2
    own = width // n
    hbm = pl.BlockSpec(memory_space=pl.ANY)
    vmem = pl.BlockSpec(memory_space=pltpu.VMEM)
    gr = heads * hd // 4
    dma = pltpu.SemaphoreType.DMA
    y, dx, dwqkv, dwo, dg, db = pl.pallas_call(
        functools.partial(kernel, n, heads, hd),
        name="block",
        out_shape=(
            jax.ShapeDtypeStruct((tokens, width), BF16), jax.ShapeDtypeStruct((tokens, width), BF16),
            jax.ShapeDtypeStruct((three * width, 128), F32), jax.ShapeDtypeStruct((own, width), F32),
            jax.ShapeDtypeStruct((width,), F32), jax.ShapeDtypeStruct((width,), F32)),
        in_specs=[hbm, hbm, vmem, vmem, hbm, hbm],
        out_specs=(hbm,) * 6,
        scratch_shapes=[
            pltpu.VMEM((tokens, width), BF16), pltpu.VMEM((tokens, width), BF16),
            pltpu.VMEM((three * width, width), BF16), pltpu.VMEM((width, width), BF16),
            pltpu.VMEM((width, tokens), BF16), pltpu.VMEM((width, tokens), BF16), pltpu.VMEM((width, tokens), BF16),
            pltpu.VMEM((three * width, tokens), BF16), pltpu.VMEM((width, tokens), BF16),
            pltpu.VMEM((1, tokens), F32), pltpu.VMEM((1, tokens), F32),
            pltpu.VMEM((width, 128), F32), pltpu.VMEM((width, 128), F32),
            pltpu.VMEM((2, gr, BLK), F32), pltpu.VMEM((2, n, hd // 2, 128), F32),
            pltpu.VMEM((2, n, hd // 2, 128), F32), pltpu.VMEM((2, n, hd // 2, 128), F32),
            pltpu.VMEM((BLK, BLK), F32), pltpu.VMEM((4, gr, gr + 16), BF16), pltpu.VMEM((4, gr + 16, gr), BF16),
            pltpu.VMEM((2, width, TT), BF16),
            pltpu.VMEM((4, chips, 2, own, width), F32), pltpu.VMEM((4, chips, own, width), F32),
            pltpu.VMEM((4, 2, own // 2, width), F32), pltpu.VMEM((4, 2, own, width), F32),
            pltpu.VMEM((width, 128), F32), pltpu.VMEM((n, 2, width), F32), pltpu.VMEM((width,), F32), pltpu.VMEM((width,), F32),
            dma((3, max(steps, 3))), dma((4, max(steps, 4))),
            dma((4, n - 1)), dma((4, n - 1)), dma((4, chips + 6)), dma((4, chips + 6)), dma((n - 1,)), dma((n - 1,)),
        ],
        compiler_params=pltpu.CompilerParams(collective_id=0, has_side_effects=True, vmem_limit_bytes=67_000_000),
    )(x_tok, dy_tok, ln_gamma, ln_beta, wt, w_out)
    return y, dx, dwqkv[:, :own].reshape(three, heads, hd, own).transpose(3, 0, 1, 2), dwo, dg, db


def solution(mesh):
    rows = P(("data", "seq"), None)
    return jax.shard_map(
        functools.partial(local_block, mesh.shape["seq"]), mesh=mesh,
        in_specs=(rows, rows, P(None), P(None), P(None, None, None, None), P(None, None)),
        out_specs=(rows, rows, P(("data", "seq"), None, None, None), rows, P("data"), P("data")),
        check_vma=False)
```

```python
import functools

import jax
import jax.numpy as jnp
from jax import lax
from jax.experimental import pallas as pl
from jax.experimental.pallas import tpu as pltpu
from jax.sharding import PartitionSpec as P

LN_EPS = 1e-5
MESH = pl.DeviceIdType.MESH
F32 = jnp.float32
BF16 = jnp.bfloat16
TT = 512
BLK = 256


def nn(a, b):
    return lax.dot_general(a, b, (((1,), (0,)), ((), ())), preferred_element_type=F32)


def nt(a, b):
    return lax.dot_general(a, b, (((1,), (1,)), ((), ())), preferred_element_type=F32)


def kernel(n, heads, hd,
           x_hbm, dy_hbm, gam_ref, bet_ref, wt_hbm, wo_hbm,
           y_hbm, dx_hbm, dwqkv_hbm, dwo_hbm, dg_hbm, db_hbm,
           xbuf, dybuf, wt, wo, xT, dyT, uT, qkvT, oT, mean_ref, rstd_ref, gb, bb,
           s_acc, comp, ar_in, ar_out, sx, sg, sgt, ubuf,
           acc, d2d, relay, fin, dgacc, dgslots, dgout, dbout,
           sem_in, sem_out, ar_send, ar_recv, rs_send, rs_recv, dg_send, dg_recv):
    tokens, width = xbuf.shape
    steps = tokens // TT
    groups = 4
    hpg = heads // groups
    gr = hpg * hd
    nb = width // BLK
    chips = n // 2
    me = lax.axis_index("seq")
    chip, core = lax.div(me, 2), lax.rem(me, 2)
    partner = 2 * chip + (1 - core)
    c_right, c_left = lax.rem(chip + 1, chips), lax.rem(chip + chips - 1, chips)
    c_opp = lax.rem(chip + 2, chips)
    right, left = 2 * c_right + core, 2 * c_left + core

    def x_copy(t):
        r = pl.ds(pl.multiple_of(t * TT, TT), TT)
        return pltpu.make_async_copy(x_hbm.at[r, :], xbuf.at[r, :], sem_in.at[0, t])

    def dy_copy(t):
        r = pl.ds(pl.multiple_of(t * TT, TT), TT)
        return pltpu.make_async_copy(dy_hbm.at[r, :], dybuf.at[r, :], sem_in.at[1, t])

    wkv_copy = pltpu.make_async_copy(wt_hbm.at[pl.ds(width, 2 * width), :], wt.at[pl.ds(width, 2 * width), :], sem_in.at[2, 0])
    wq_copy = pltpu.make_async_copy(wt_hbm.at[pl.ds(0, width), :], wt.at[pl.ds(0, width), :], sem_in.at[2, 1])
    wo_copy = pltpu.make_async_copy(wo_hbm, wo, sem_in.at[2, 2])
    x_copy(0).start()
    wkv_copy.start()
    for t in range(1, steps):
        x_copy(t).start()
    for t in range(steps):
        dy_copy(t).start()
    wq_copy.start()
    wo_copy.start()

    barrier = pltpu.get_barrier_semaphore()
    for d in range(1, n):
        pl.semaphore_signal(barrier, inc=1, device_id={"seq": lax.rem(me + d, n)}, device_id_type=MESH)

    eye = (lax.broadcasted_iota(jnp.int32, (BLK, BLK), 0) == lax.broadcasted_iota(jnp.int32, (BLK, BLK), 1)).astype(F32).astype(BF16)
    gb[...] = jnp.transpose(jnp.broadcast_to(gam_ref[...][None, :], (128, width)))
    bb[...] = jnp.transpose(jnp.broadcast_to(bet_ref[...][None, :], (128, width)))
    s_acc[...] = jnp.zeros_like(s_acc)
    sx[...] = jnp.zeros_like(sx)
    dgacc[...] = jnp.zeros_like(dgacc)

    def lanes(ref_val, tt=TT):
        return jnp.concatenate([ref_val] * (tt // 128), axis=1)

    def fold(v):
        out = v[:, :128]
        for i in range(1, TT // 128):
            out = out + v[:, 128 * i:128 * (i + 1)]
        return out

    def tok(t, tt=TT):
        return pl.ds(t * tt if isinstance(t, int) else pl.multiple_of(t * tt, tt), tt)

    def phi(v32):
        ex = jnp.exp(jnp.minimum(v32, 0.0))
        pos = v32 > 0
        return jnp.where(pos, v32 + 1.0, ex).astype(BF16), jnp.where(pos, 1.0, ex)

    def parts3(v):
        p1 = v.astype(BF16).astype(F32)
        r = v - p1
        p2 = r.astype(BF16).astype(F32)
        return p1, p2, (r - p2).astype(BF16).astype(F32)

    scope = jax.named_scope
    ones_rows = jnp.ones((BLK - gr, TT), BF16)

    def norm_tile(t):
        ts = tok(t)
        xt = jnp.concatenate([nt(eye, xbuf[ts, BLK * b:BLK * (b + 1)]) for b in range(nb)], axis=0)
        xT[:, ts] = xt.astype(BF16)
        mean = jnp.sum(xt, axis=0, keepdims=True) * (1.0 / width)
        cen = xt - mean
        var = jnp.sum(cen * cen, axis=0, keepdims=True) * (1.0 / width)
        rstd = lax.rsqrt(var + LN_EPS)
        mean_ref[:, ts] = mean
        rstd_ref[:, ts] = rstd
        u = (cen * rstd * lanes(gb[...]) + lanes(bb[...])).astype(BF16)
        uT[:, ts] = u
        ubuf[t % 2] = u

    def kv_mm(t, half, u):
        ts = tok(t)
        hw = width // 2
        kb = nn(wt[width + hw * half:width + hw * (half + 1), :], u[...]).astype(BF16)
        vb = nn(wt[2 * width + hw * half:2 * width + hw * (half + 1), :], u[...]).astype(BF16)
        qkvT[width + hw * half:width + hw * (half + 1), ts] = kb
        qkvT[2 * width + hw * half:2 * width + hw * (half + 1), ts] = vb
        return half, phi(kb.astype(F32))[0], vb

    def s_mm(half, fk, vb):
        for i, g in enumerate(half_groups(half)):
            rows = slice(gr * i, gr * (i + 1))
            s_acc[g % 2] += nt(fk[rows], jnp.concatenate([vb[rows], ones_rows], axis=0))

    def half_groups(half):
        return range(groups // 2 * half, groups // 2 * (half + 1))

    lane128 = lax.broadcasted_iota(jnp.int32, (hd, 128), 1)
    lane256 = lax.broadcasted_iota(jnp.int32, (hd, BLK), 1)
    lane_sx = lax.broadcasted_iota(jnp.int32, (BLK, BLK), 1)
    rows_owned = hd // 2

    def compact(e, z_of):
        g0 = groups // 2 * (e % 2)

        def head(g, hh):
            blk = s_acc[g % 2, hd * hh:hd * (hh + 1), :]
            moved = pltpu.roll(blk, BLK - hd * hh, axis=1) if hh else blk
            return jnp.where(lane128 < hd, moved[:, :128], jnp.where(lane128 == hd, z_of(hh, blk), 0.0))

        if e >= 2:
            for d in range(1, n):
                ar1(e - 2, d).wait_send()
        for j in range(hpg):
            pair = head(g0, j) + pltpu.roll(head(g0 + 1, j), 64, axis=1)
            comp[e % 2, 2 * j] = pair[:rows_owned]
            comp[e % 2, 2 * j + 1] = pair[rows_owned:]
        s_acc[...] = jnp.zeros_like(s_acc)
        for d in range(1, n):
            ar1(e, d).start()

    def ar1(e, d):
        peer = lax.rem(me + d, n)
        return pltpu.make_async_remote_copy(
            src_ref=comp.at[e % 2, peer], dst_ref=ar_in.at[e % 2, d], send_sem=ar_send.at[2 * (e % 2), d - 1], recv_sem=ar_recv.at[2 * (e % 2), d - 1],
            device_id={"seq": peer}, device_id_type=MESH)

    def ar2(e, d):
        peer = lax.rem(me + d, n)
        return pltpu.make_async_remote_copy(
            src_ref=ar_out.at[e % 2, 0], dst_ref=ar_out.at[e % 2, d], send_sem=ar_send.at[2 * (e % 2) + 1, d - 1], recv_sem=ar_recv.at[2 * (e % 2) + 1, d - 1],
            device_id={"seq": peer}, device_id_type=MESH)

    def ar_reduce(e):
        total = comp[e % 2, me]
        for d in range(1, n):
            ar1(e, d).wait_recv()
            total = total + ar_in[e % 2, d]
            if e >= 2:
                ar2(e - 2, d).wait_send()
        ar_out[e % 2, 0] = total
        for d in range(1, n):
            ar2(e, d).start()

    def ar_finish(i):
        forward = i < 2
        for d in range(1, n):
            ar2(i, d).wait_recv()
        for g in half_groups(i % 2):
            for hh in range(hpg):
                part = jnp.concatenate([ar_out[i % 2, lax.rem(me - p + n, n)] for p in (2 * hh, 2 * hh + 1)], axis=0)
                if g % 2:
                    part = pltpu.roll(part, 64, axis=1)
                wide = jnp.concatenate([jnp.where(lane128 < hd, part, 0.0), jnp.zeros((hd, 128), F32)], axis=1)
                if hh:
                    wide = pltpu.roll(wide, hd * hh, axis=1)
                zc = part[:, hd:hd + 1]
                if forward:
                    hit = (lane256 == gr + hh) | (lane256 == gr + hpg + hh) | (lane256 == gr + 2 * hpg + hh)
                    wide = jnp.where(hit, jnp.broadcast_to(zc, (hd, BLK)), wide)
                else:
                    for j, zp in enumerate(parts3(jnp.broadcast_to(zc, (hd, BLK)))):
                        wide = jnp.where(lane256 == gr + j, zp, wide)
                sx[hd * hh:hd * (hh + 1), :] = wide
            m = sx[...]
            ext = jnp.where(lane_sx >= gr, -m, m) if forward else m
            sg[g] = ext[:gr, :gr + 16].astype(BF16)
            sgt[g] = jnp.transpose(m)[:gr + 16, :gr].astype(BF16)

    def z_fwd(hh, blk):
        return blk[:, gr:gr + 1]

    off = lane128 - (gr - 128)

    def z_bwd(hh, blk):
        hit = (off >= 0) & (off < 3 * hpg) & (lax.rem(off, hpg) == hh)
        return -jnp.sum(jnp.where(hit, blk[:, 128:], 0.0), axis=1, keepdims=True)

    def do_tile(t):
        acc[t, pl.ds(0, 2), :, :, :TT] = nn(wo[:width // 2, :], dyT[:, tok(t)]).reshape(2, 2, gr // 2, TT)

    def q_tile(t):
        ts = tok(t)
        dy_copy(t).wait()
        for b in range(nb):
            dyT[BLK * b:BLK * (b + 1), ts] = nt(eye, dybuf[ts, BLK * b:BLK * (b + 1)]).astype(BF16)
        qkvT[0:width, ts] = nn(wt[0:width, :], uT[:, ts]).astype(BF16)

    with scope("A0"):
        x_copy(0).wait()
        norm_tile(0)
    wkv_copy.wait()
    for t in range(steps):
        with scope(f"A_{t}"):
            if t + 1 < steps:
                x_copy(t + 1).wait()
                norm_tile(t + 1)
            now = kv_mm(t, 0, ubuf.at[t % 2])
            if t:
                s_mm(*last)
            last = now
    with scope("A_s"):
        s_mm(*last)
    pl.semaphore_wait(barrier, n - 1)
    with scope("compact0"):
        compact(0, z_fwd)
    with scope("A2"):
        @pl.loop(0, steps)
        def _(t):
            s_mm(*kv_mm(t, 1, uT.at[:, tok(t)]))
    with scope("compact1"):
        compact(1, z_fwd)

    wq_copy.wait()
    with scope("fill_q0"):
        q_tile(0)
    with scope("ar_reduce0"):
        ar_reduce(0)
    with scope("fill_q1"):
        pl.loop(1, steps)(q_tile)
    wo_copy.wait()
    with scope("do0"):
        pl.loop(0, steps)(do_tile)
    with scope("ar_reduce1"):
        ar_reduce(1)
    with scope("ar_finish0"):
        ar_finish(0)

    def per_head(v):
        return jnp.broadcast_to(v[:, None, :], (hpg, hd, TT)).reshape(gr, TT)

    def o_tiles(i, half):
        nds = [nn(sgt[g], phi(qkvT[gr * g:gr * (g + 1), tok(i)].astype(F32))[0]) for g in half_groups(half)]
        for g, nd in zip(half_groups(half), nds):
            oT[gr * g:gr * (g + 1), tok(i)] = (nd[:gr] * per_head(1.0 / nd[gr:gr + hpg])).astype(BF16)

    def b_tiles(i, half):
        pairs = [(i, g) for g in half_groups(half)]
        rows = {g: slice(gr * g, gr * (g + 1)) for _, g in pairs}
        feats = [phi(qkvT[rows[g], tok(t)].astype(F32)) for t, g in pairs]
        nds = [nn(sgt[g], fq) for (t, g), (fq, _) in zip(pairs, feats)]
        dos = [acc[t, g, :, :, :TT].reshape(gr, TT) if half == 0 else nn(wo[rows[g], :], dyT[:, tok(t)]) for t, g in pairs]
        ges = []
        for (t, g), nd, do in zip(pairs, nds, dos):
            rden = per_head(1.0 / nd[gr:gr + hpg])
            a = nd[:gr] * rden
            if half == 0:
                oT[rows[g], tok(t)] = a.astype(BF16)
            gg = (do * rden).astype(BF16)
            c = jnp.sum((gg.astype(F32) * a).reshape(hpg, hd, TT), axis=1)
            cp = jnp.concatenate(list(parts3(c)) + [jnp.zeros((hpg, TT), F32)], axis=0).astype(BF16)
            ges.append(jnp.concatenate([gg, cp], axis=0))
        dfqs = [nn(sg[g], ge) for (t, g), ge in zip(pairs, ges)]
        for (t, g), (fq, slope), ge, dfq in zip(pairs, feats, ges, dfqs):
            s_acc[g % 2] += nt(fq, jnp.concatenate([ge, jnp.zeros((BLK - gr - 16, TT), BF16)], axis=0))
            qkvT[rows[g], tok(t)] = (dfq * slope).astype(BF16)

    own = width // n

    def grad(u, between=None):
        @pl.loop(0, 2)
        def _(m):
            if between is not None:
                pl.when(m == 1)(between)
            half = lax.rem(lax.div(chip, 2) + 1 + m, 2)
            rs = pl.ds(pl.multiple_of(half * (width // 2), width // 2), width // 2)
            if u == 0:
                out = nn(oT[rs, :], dybuf[...])
            else:
                out = nt(uT[rs, :], qkvT[width * (u - 1):width * u, :])
            acc[u, pl.ds(2 * half, 2)] = out.reshape(2, 2, own, width)
            d2d_copy(u, 2 * half).start()
            d2d_copy(u, 2 * half + 1).start()

    hr = width // n // 2
    lo, hi = pl.ds(0, hr), pl.ds(hr, hr)

    def rdma(u, s, src, dst, peer):
        return pltpu.make_async_remote_copy(src_ref=src, dst_ref=dst, send_sem=rs_send.at[u, s], recv_sem=rs_recv.at[u, s],
                                            device_id={"seq": peer}, device_id_type=MESH)

    def d2d_copy(u, c):
        return rdma(u, c, acc.at[u, c, 1 - core], d2d.at[u, c], partner)

    def hop(u, s):
        if s == 0:
            return rdma(u, chips, acc.at[u, c_opp, core, lo], relay.at[u, 0], right)
        if s == 1:
            return rdma(u, chips + 1, acc.at[u, c_opp, core, hi], relay.at[u, 1], left)
        if s == 2:
            return rdma(u, chips + 2, acc.at[u, c_right, core, hi], fin.at[u, 0, hi], right)
        if s == 3:
            return rdma(u, chips + 3, acc.at[u, c_left, core, lo], fin.at[u, 1, lo], left)
        if s == 4:
            return rdma(u, chips + 4, acc.at[u, c_right, core, lo], fin.at[u, 0, lo], right)
        return rdma(u, chips + 5, acc.at[u, c_left, core, hi], fin.at[u, 1, hi], left)

    def rs_chip_a(u):
        d2d_copy(u, c_opp).wait_recv()
        acc[u, c_opp, core] += d2d[u, c_opp]
        hop(u, 0).start()
        hop(u, 1).start()

    def rs_chip_b(u):
        d2d_copy(u, c_right).wait_recv()
        acc[u, c_right, core] += d2d[u, c_right]
        hop(u, 2).start()
        d2d_copy(u, c_left).wait_recv()
        acc[u, c_left, core] += d2d[u, c_left]
        hop(u, 3).start()
        d2d_copy(u, chip).wait_recv()
        acc[u, chip, core] += d2d[u, chip]

    def rs_relay(u):
        hop(u, 0).wait_recv()
        acc[u, c_right, core, lo] += relay[u, 0]
        hop(u, 4).start()
        hop(u, 1).wait_recv()
        acc[u, c_left, core, hi] += relay[u, 1]
        hop(u, 5).start()

    def out_copy(u):
        if u == 0:
            return pltpu.make_async_copy(acc.at[u, chip, core], dwo_hbm, sem_out.at[2, u])
        return pltpu.make_async_copy((gb, dgacc, bb)[u - 1], dwqkv_hbm.at[pl.ds(width * (u - 1), width), :], sem_out.at[2, u])

    def rs_final(u):
        for s in range(2, 6):
            hop(u, s).wait_recv()
        total = acc[u, chip, core] + fin[u, 0] + fin[u, 1]
        if u == 0:
            acc[u, chip, core] = total
        else:
            (gb, dgacc, bb)[u - 1][:, :own] = jnp.transpose(total)
        out_copy(u).start()

    def y_copy(t):
        r = tok(t)
        return pltpu.make_async_copy(xbuf.at[r, :], y_hbm.at[r, :], sem_out.at[0, t])

    def dx_copy(t):
        r = tok(t)
        return pltpu.make_async_copy(dybuf.at[r, :], dx_hbm.at[r, :], sem_out.at[1, t])

    def store_tokens(buf, t, val):
        for s in range(TT // BLK):
            r = pl.ds(t * TT + BLK * s if isinstance(t, int) else pl.multiple_of(t * TT + BLK * s, BLK), BLK)
            for b in range(nb):
                buf[r, BLK * b:BLK * (b + 1)] = nt(eye, val[BLK * b:BLK * (b + 1), BLK * s:BLK * (s + 1)]).astype(BF16)

    def y_tile(t):
        ts = tok(t)
        yt = (nn(ubuf[0], oT[:TT, ts]) + nn(ubuf[1, :, :width - TT], oT[TT:, ts]) + xT[:, ts].astype(F32)).astype(BF16)
        store_tokens(xbuf, t, yt)
        y_copy(t).start()

    def c_tiles(i, half):
        pairs = [(2 * i + k, g) for k in range(2) for g in half_groups(half)]
        krows = {g: slice(width + gr * g, width + gr * (g + 1)) for _, g in pairs}
        vrows = {g: slice(2 * width + gr * g, 2 * width + gr * (g + 1)) for _, g in pairs}
        dfks = [nn(sg[g], jnp.concatenate([qkvT[vrows[g], tok(t)], ones_rows[:16]], axis=0)) for t, g in pairs]
        feats = [phi(qkvT[krows[g], tok(t)].astype(F32)) for t, g in pairs]
        dvs = [nn(sgt[g, :gr, :], fk) for (t, g), (fk, _) in zip(pairs, feats)]
        for (t, g), (_, slope), dfk, dv in zip(pairs, feats, dfks, dvs):
            qkvT[krows[g], tok(t)] = (dfk * slope).astype(BF16)
            qkvT[vrows[g], tok(t)] = dv.astype(BF16)

    def du_tile(t):
        i = 2 * (t % 2)
        d2d[i:i + 2, :, :, :TT] = (nn(dyT[...], qkvT[:tokens, tok(t)]) + nn(ubuf[1, :, BLK:], qkvT[tokens:, tok(t)])).reshape(2, chips, own, TT)

    def dx_tile(t):
        ts = tok(t)
        i = 2 * (t % 2)
        du = d2d[i:i + 2, :, :, :TT].reshape(width, TT)
        rstd = rstd_ref[:, ts]
        xhat = (xT[:, ts].astype(F32) - mean_ref[:, ts]) * rstd
        p = du * xhat
        dgacc[...] += fold(p)
        bb[...] += fold(du)
        gl = lanes(gb[...])
        e = du * gl
        m1 = jnp.sum(e, axis=0, keepdims=True) * (1.0 / width)
        m2 = jnp.sum(p * gl, axis=0, keepdims=True) * (1.0 / width)
        dxt = (uT[:, ts].astype(F32) + rstd * (e - m1 - xhat * m2)).astype(BF16)
        store_tokens(dybuf, t, dxt)

    def w_block(j):
        js = pl.ds(pl.multiple_of(j * BLK, BLK), BLK)
        for i in range(nb):
            dyT[BLK * i:BLK * (i + 1), js] = nt(eye, wt[js, BLK * i:BLK * (i + 1)]).astype(BF16)

    def w_rest():
        for i in range(nb):
            ubuf[1, BLK * i:BLK * (i + 1), BLK:] = nt(eye, wt[tokens:, BLK * i:BLK * (i + 1)]).astype(BF16)

    with scope("B0"):
        pl.loop(0, steps)(functools.partial(b_tiles, half=0))
    with scope("compact2"):
        compact(2, z_bwd)
    with scope("ar_finish1"):
        ar_finish(1)
    with scope("O1"):
        pl.loop(0, steps)(functools.partial(o_tiles, half=1))
    with scope("gradwo"):
        grad(0)
    with scope("ar_reduce2"):
        ar_reduce(2)
    with scope("rs_chip_a0"):
        rs_chip_a(0)
    with scope("B1"):
        @pl.loop(0, steps)
        def _(t):
            @pl.when(t == steps // 2)
            def _():
                rs_chip_b(0)
            b_tiles(t, half=1)
    with scope("compact3"):
        compact(3, z_bwd)
    with scope("fill_w"):
        pl.loop(0, tokens // BLK)(w_block)
        w_rest()
    with scope("relay0"):
        rs_relay(0)
    with scope("gradwq"):
        grad(1)
    with scope("ar_reduce3"):
        ar_reduce(3)
    with scope("chip_a1"):
        rs_chip_a(1)
    with scope("ar_finish2"):
        ar_finish(2)
    with scope("C0"):
        pl.loop(0, steps // 2)(functools.partial(c_tiles, half=0))
    with scope("rs_chip_b1"):
        rs_chip_b(1)
    with scope("fill_wo"):
        for i in range(nb):
            for j in range(nb):
                k = BLK * i // TT
                ubuf[k, BLK * j:BLK * (j + 1), BLK * i - TT * k:BLK * (i + 1) - TT * k] = nt(
                    eye, wo[BLK * i:BLK * (i + 1), BLK * j:BLK * (j + 1)]).astype(BF16)
    with scope("Y0"):
        pl.loop(0, steps // 4)(y_tile)
    with scope("ar_finish3"):
        ar_finish(3)
    with scope("C1"):
        pl.loop(0, steps // 2)(functools.partial(c_tiles, half=1))
    with scope("relay1"):
        rs_relay(1)
    with scope("gradwk"):
        grad(2)
    with scope("rs_chip_a2"):
        rs_chip_a(2)
    with scope("gradwv"):
        grad(3, lambda: rs_chip_b(2))
    with scope("rs_chip_a3"):
        rs_chip_a(3)
    bb[...] = jnp.zeros_like(bb)
    for t in range(steps + 1):
        with scope(f"DU_{t}"):
            if t > 0:
                for b in range(nb):
                    uT[BLK * b:BLK * (b + 1), tok(t - 1)] = nt(eye, dybuf[tok(t - 1), BLK * b:BLK * (b + 1)]).astype(BF16)
            if t < steps:
                du_tile(t)
            if t > 0:
                dx_tile(t - 1)
                dx_copy(t - 1).start()
        if t == 0:
            with scope("relay2"):
                rs_chip_b(3)
                rs_relay(2)
        if t == 2:
            with scope("relay3"):
                rs_relay(3)

    def dg_copy(d):
        return pltpu.make_async_remote_copy(
            src_ref=dgslots.at[0], dst_ref=dgslots.at[d], send_sem=dg_send.at[d - 1], recv_sem=dg_recv.at[d - 1],
            device_id={"seq": lax.rem(me + d, n)}, device_id_type=MESH)

    dgrow = jnp.sum(jnp.transpose(dgacc[...]), axis=0, keepdims=True)
    dbrow = jnp.sum(jnp.transpose(bb[...]), axis=0, keepdims=True)
    dgslots[0] = jnp.concatenate([dgrow, dbrow], axis=0)
    for d in range(1, n):
        dg_copy(d).start()

    def dg_out(i):
        return pltpu.make_async_copy((dgout, dbout)[i], (dg_hbm, db_hbm)[i], sem_out.at[3, i])

    with scope("final"):
        rs_final(0)
        rs_final(1)
    with scope("Y1"):
        pl.loop(steps // 4, steps)(y_tile)
    with scope("final2"):
        rs_final(2)
    with scope("final3"):
        rs_final(3)

    with scope("dg"):
        for d in range(1, n):
            dg_copy(d).wait_recv()
        total = dgslots[me]
        for p in range(1, n):
            total = total + dgslots[lax.rem(me - p + n, n)]
        dgout[...] = total[0]
        dbout[...] = total[1]
        dg_out(0).start()
        dg_out(1).start()
    dg_out(0).wait()
    dg_out(1).wait()
    for d in range(1, n):
        for e in (2, 3):
            ar1(e, d).wait_send()
            ar2(e, d).wait_send()
        dg_copy(d).wait_send()
    for u in range(4):
        out_copy(u).wait()
        for c in range(chips):
            d2d_copy(u, c).wait_send()
        for s in range(6):
            hop(u, s).wait_send()

    @pl.loop(0, steps)
    def _(t):
        y_copy(t).wait()
        dx_copy(t).wait()


def local_block(n, x_tok, dy_tok, ln_gamma, ln_beta, w_qkv, w_out):
    tokens, width = x_tok.shape
    _, three, heads, hd = w_qkv.shape
    wt = w_qkv.transpose(1, 2, 3, 0).reshape(three * width, width)
    steps = tokens // TT
    chips = n // 2
    own = width // n
    hbm = pl.BlockSpec(memory_space=pl.ANY)
    vmem = pl.BlockSpec(memory_space=pltpu.VMEM)
    gr = heads * hd // 4
    dma = pltpu.SemaphoreType.DMA
    y, dx, dwqkv, dwo, dg, db = pl.pallas_call(
        functools.partial(kernel, n, heads, hd),
        name="block",
        out_shape=(
            jax.ShapeDtypeStruct((tokens, width), BF16), jax.ShapeDtypeStruct((tokens, width), BF16),
            jax.ShapeDtypeStruct((three * width, 128), F32), jax.ShapeDtypeStruct((own, width), F32),
            jax.ShapeDtypeStruct((width,), F32), jax.ShapeDtypeStruct((width,), F32)),
        in_specs=[hbm, hbm, vmem, vmem, hbm, hbm],
        out_specs=(hbm,) * 6,
        scratch_shapes=[
            pltpu.VMEM((tokens, width), BF16), pltpu.VMEM((tokens, width), BF16),
            pltpu.VMEM((three * width, width), BF16), pltpu.VMEM((width, width), BF16),
            pltpu.VMEM((width, tokens), BF16), pltpu.VMEM((width, tokens), BF16), pltpu.VMEM((width, tokens), BF16),
            pltpu.VMEM((three * width, tokens), BF16), pltpu.VMEM((width, tokens), BF16),
            pltpu.VMEM((1, tokens), F32), pltpu.VMEM((1, tokens), F32),
            pltpu.VMEM((width, 128), F32), pltpu.VMEM((width, 128), F32),
            pltpu.VMEM((2, gr, BLK), F32), pltpu.VMEM((2, n, hd // 2, 128), F32),
            pltpu.VMEM((2, n, hd // 2, 128), F32), pltpu.VMEM((2, n, hd // 2, 128), F32),
            pltpu.VMEM((BLK, BLK), F32), pltpu.VMEM((4, gr, gr + 16), BF16), pltpu.VMEM((4, gr + 16, gr), BF16),
            pltpu.VMEM((2, width, TT), BF16),
            pltpu.VMEM((4, chips, 2, own, width), F32), pltpu.VMEM((4, chips, own, width), F32),
            pltpu.VMEM((4, 2, own // 2, width), F32), pltpu.VMEM((4, 2, own, width), F32),
            pltpu.VMEM((width, 128), F32), pltpu.VMEM((n, 2, width), F32), pltpu.VMEM((width,), F32), pltpu.VMEM((width,), F32),
            dma((3, max(steps, 3))), dma((4, max(steps, 4))),
            dma((4, n - 1)), dma((4, n - 1)), dma((4, chips + 6)), dma((4, chips + 6)), dma((n - 1,)), dma((n - 1,)),
        ],
        compiler_params=pltpu.CompilerParams(collective_id=0, has_side_effects=True, vmem_limit_bytes=67_000_000),
    )(x_tok, dy_tok, ln_gamma, ln_beta, wt, w_out)
    return y, dx, dwqkv[:, :own].reshape(three, heads, hd, own).transpose(3, 0, 1, 2), dwo, dg, db


def solution(mesh):
    rows = P(("data", "seq"), None)
    return jax.shard_map(
        functools.partial(local_block, mesh.shape["seq"]), mesh=mesh,
        in_specs=(rows, rows, P(None), P(None), P(None, None, None, None), P(None, None)),
        out_specs=(rows, rows, P(("data", "seq"), None, None, None), rows, P("data"), P("data")),
        check_vma=False)
```
